32 devices in a mesh: z: 4 (over z), y: 2 (over y), x: 4 (over x, core).
Axes of the slice: x: 2, y: 2, z: 4, core: 2. Of those that a mesh axis runs over, the one named last changes fastest.
Arguments:
- x_in: bfloat16 [65536, 4096], P(('z', 'y', 'x'))
- g_out: bfloat16 [65536, 512], P(('z', 'y', 'x'))
- w_in: bfloat16 [4096, 512], replicated
- w_up1: bfloat16 [512, 2048], replicated
- w_down1: bfloat16 [2048, 512], replicated
- w_up2: bfloat16 [512, 2048], replicated
- w_down2: bfloat16 [2048, 512], replicated
Outputs:
- output 1: bfloat16 [65536, 4096], P(('z', 'y', 'x'))
- output 2: float32 [4096, 512], replicated
- output 3: float32 [512, 2048], replicated
- output 4: float32 [2048, 512], replicated
- output 5: float32 [512, 2048], replicated
- output 6: float32 [2048, 512], replicated
All inputs are finite; a program needn't handle non-finite values.
Results may differ from the reference program's by a relative error of at most 0.0133355.
Values are sent between devices in bfloat16 or wider.
A program may use at most 1 GiB of HBM per device.

```python
import jax
import jax.numpy as jnp
from jax import lax

D_MODEL = 512
D_FF = 2048
D_IN = 4096
TOK_DEV = 2048
N_DEVICES = 32

TOKENS = TOK_DEV * N_DEVICES
SQRT_HALF = 0.7071067811865476
INV_SQRT_TAU = 0.3989422804014327


def gelu_value(pre_act):
    pre_wide = pre_act.astype(jnp.float32)
    return 0.5 * pre_wide * (1.0 + lax.erf(pre_wide * SQRT_HALF))


def gelu_slope(pre_act):
    pre_wide = pre_act.astype(jnp.float32)
    return 0.5 * (1.0 + lax.erf(pre_wide * SQRT_HALF)) + pre_wide * jnp.exp(-0.5 * pre_wide * pre_wide) * INV_SQRT_TAU


def setup_inputs(seed: int = 0) -> dict:
    keys = jax.random.split(jax.random.key(seed), 7)
    x_in = jax.random.normal(keys[0], (TOKENS, D_IN), jnp.float32)
    g_out = jax.random.normal(keys[1], (TOKENS, D_MODEL), jnp.float32)
    w_in = jax.random.normal(keys[2], (D_IN, D_MODEL), jnp.float32) * D_IN ** -0.5
    w_up1 = jax.random.normal(keys[3], (D_MODEL, D_FF), jnp.float32) * D_MODEL ** -0.5
    w_down1 = jax.random.normal(keys[4], (D_FF, D_MODEL), jnp.float32) * D_FF ** -0.5
    w_up2 = jax.random.normal(keys[5], (D_MODEL, D_FF), jnp.float32) * D_MODEL ** -0.5
    w_down2 = jax.random.normal(keys[6], (D_FF, D_MODEL), jnp.float32) * D_FF ** -0.5
    return {
        "x_in": x_in.astype(jnp.bfloat16),
        "g_out": g_out.astype(jnp.bfloat16),
        "w_in": w_in.astype(jnp.bfloat16),
        "w_up1": w_up1.astype(jnp.bfloat16),
        "w_down1": w_down1.astype(jnp.bfloat16),
        "w_up2": w_up2.astype(jnp.bfloat16),
        "w_down2": w_down2.astype(jnp.bfloat16),
    }


def local_backward(x_in, g_out, w_in, w_up1, w_down1, w_up2, w_down2):
    x_mid = jnp.dot(x_in, w_in, preferred_element_type=jnp.float32).astype(jnp.bfloat16)
    pre_one = jnp.dot(x_mid, w_up1, preferred_element_type=jnp.float32).astype(jnp.bfloat16)
    act_one = gelu_value(pre_one).astype(jnp.bfloat16)
    hid_two = (jnp.dot(act_one, w_down1, preferred_element_type=jnp.float32) + x_mid.astype(jnp.float32)).astype(jnp.bfloat16)
    pre_three = jnp.dot(hid_two, w_up2, preferred_element_type=jnp.float32).astype(jnp.bfloat16)
    act_three = gelu_value(pre_three).astype(jnp.bfloat16)
    grad_down2 = jnp.dot(act_three.T, g_out, preferred_element_type=jnp.float32)
    d_act3 = jnp.dot(g_out, w_down2.T, preferred_element_type=jnp.float32).astype(jnp.bfloat16)
    d_pre3 = (d_act3.astype(jnp.float32) * gelu_slope(pre_three)).astype(jnp.bfloat16)
    grad_up2 = jnp.dot(hid_two.T, d_pre3, preferred_element_type=jnp.float32)
    d_hid2 = (jnp.dot(d_pre3, w_up2.T, preferred_element_type=jnp.float32) + g_out.astype(jnp.float32)).astype(jnp.bfloat16)
    grad_down1 = jnp.dot(act_one.T, d_hid2, preferred_element_type=jnp.float32)
    d_act1 = jnp.dot(d_hid2, w_down1.T, preferred_element_type=jnp.float32).astype(jnp.bfloat16)
    d_pre1 = (d_act1.astype(jnp.float32) * gelu_slope(pre_one)).astype(jnp.bfloat16)
    grad_up1 = jnp.dot(x_mid.T, d_pre1, preferred_element_type=jnp.float32)
    d_mid = (jnp.dot(d_pre1, w_up1.T, preferred_element_type=jnp.float32) + d_hid2.astype(jnp.float32)).astype(jnp.bfloat16)
    grad_in = jnp.dot(x_in.T, d_mid, preferred_element_type=jnp.float32)
    dx_rows = jnp.dot(d_mid, w_in.T, preferred_element_type=jnp.float32).astype(jnp.bfloat16)
    return dx_rows, (grad_in, grad_up1, grad_down1, grad_up2, grad_down2)


def reference(x_in, g_out, w_in, w_up1, w_down1, w_up2, w_down2):
    x_shards = x_in.reshape(N_DEVICES, TOK_DEV, D_IN)
    g_shards = g_out.reshape(N_DEVICES, TOK_DEV, D_MODEL)
    zero_sums = (
        jnp.zeros((D_IN, D_MODEL), jnp.float32),
        jnp.zeros((D_MODEL, D_FF), jnp.float32),
        jnp.zeros((D_FF, D_MODEL), jnp.float32),
        jnp.zeros((D_MODEL, D_FF), jnp.float32),
        jnp.zeros((D_FF, D_MODEL), jnp.float32),
    )

    def shard_step(partial_sums, shard):
        dx_rows, grads = local_backward(shard[0], shard[1], w_in, w_up1, w_down1, w_up2, w_down2)
        return tuple(total + piece for total, piece in zip(partial_sums, grads)), dx_rows

    totals, dx_parts = lax.scan(shard_step, zero_sums, (x_shards, g_shards))
    scale = 1.0 / N_DEVICES
    return (dx_parts.reshape(TOKENS, D_IN), totals[0] * scale, totals[1] * scale, totals[2] * scale, totals[3] * scale, totals[4] * scale)
```

```python
import functools
import jax
import jax.numpy as jnp
from jax import lax
from jax.experimental import pallas as pl
from jax.experimental.pallas import tpu as pltpu
from jax.sharding import PartitionSpec as P

SQRT_HALF = 0.7071067811865476
INV_SQRT_TAU = 0.3989422804014327
MESH = pl.DeviceIdType.MESH
F32 = jnp.float32
BF16 = jnp.bfloat16

SIDE = 512
SLOTS = 24
STAGES = 10
LAG = (0, 1, 2, 3, 4, 5, 6, 7, 8, 9)


def gelu_value(pre_act):
    pre_wide = pre_act.astype(jnp.float32)
    return 0.5 * pre_wide * (1.0 + lax.erf(pre_wide * SQRT_HALF))


def gelu_slope(pre_act):
    pre_wide = pre_act.astype(jnp.float32)
    return 0.5 * (1.0 + lax.erf(pre_wide * SQRT_HALF)) + pre_wide * jnp.exp(-0.5 * pre_wide * pre_wide) * INV_SQRT_TAU


def plain_product(first_op, second_op):
    return lax.dot_general(first_op, second_op, (((1,), (0,)), ((), ())), preferred_element_type=jnp.float32)


def rows_contract(first_op, second_op):
    return lax.dot_general(first_op, second_op, (((0,), (0,)), ((), ())), preferred_element_type=jnp.float32)


def times_transposed(first_op, second_op):
    return lax.dot_general(first_op, second_op, (((1,), (1,)), ((), ())), preferred_element_type=jnp.float32)


def blocks_of(shape):
    rows, cols = shape
    return [(r, c) for r in range(0, rows, SIDE) for c in range(0, cols, SIDE)]


def add_rows(dst, dst_row, src, src_row, count, scale=None):
    step = 16

    def body(i, _):
        at = pl.ds(pl.multiple_of(dst_row + i * step, step), step)
        value = dst[at, :] + src[pl.ds(pl.multiple_of(src_row + i * step, step), step), :]
        dst[at, :] = value if scale is None else value * scale
        return 0

    lax.fori_loop(0, count // step, body, 0, unroll=True)


class Exchange:
    def __init__(self, total, scale, part, r0, r1, r2, r3, r4, send, recv, free, ready, emit):
        self.free = free
        self.total, self.scale, self.part = total, scale, part
        self.r0, self.r1, self.r2, self.r3, self.r4 = r0, r1, r2, r3, r4
        self.send, self.recv, self.ready, self.emit = send, recv, ready, emit
        z, y, x = lax.axis_index("z"), lax.axis_index("y"), lax.axis_index("x")
        core, chip = lax.rem(x, 2), x // 2
        self.z = z
        self.core_peer = (z, y, chip * 2 + 1 - core)
        self.x_peer = (z, y, (1 - chip) * 2 + core)
        self.y_peer = (z, 1 - y, x)
        self.inner = (z >= 1) & (z <= 2)
        self.outer = (z == 0) | (z == 3)
        self.mid = jnp.where(z >= 2, 1, 0)
        self.z_inner = (jnp.where(z == 0, 1, 2), y, x)
        self.z_peer = (jnp.where(z == 1, 2, 1), y, x)
        self.z_outer = (jnp.where(z == 1, 0, 3), y, x)
        half = SIDE // 2
        self.own = core * half
        self.other = (1 - core) * half
        self.a = self.own + chip * (half // 4)
        self.a_far = self.own + (1 - chip) * (half // 4)
        self.b = self.own + half // 2 + y * (half // 4)
        self.b_far = self.own + half // 2 + (1 - y) * (half // 4)

    def barrier(self):
        sem = pltpu.get_barrier_semaphore()
        for peer in (self.core_peer, self.x_peer, self.y_peer):
            pl.semaphore_signal(sem, inc=1, device_id=peer, device_id_type=MESH)

        @pl.when(self.inner)
        def _():
            pl.semaphore_signal(sem, inc=1, device_id=self.z_peer, device_id_type=MESH)
            pl.semaphore_signal(sem, inc=1, device_id=self.z_outer, device_id_type=MESH)
            pl.semaphore_wait(sem, 5)

        @pl.when(self.outer)
        def _():
            pl.semaphore_signal(sem, inc=1, device_id=self.z_inner, device_id_type=MESH)
            pl.semaphore_wait(sem, 4)

    def copy(self, kind, k, src, dst, peer):
        return pltpu.make_async_remote_copy(
            src_ref=src, dst_ref=dst, send_sem=self.send.at[kind, k], recv_sem=self.recv.at[kind, k],
            device_id=peer, device_id_type=MESH)

    def rows(self, k, start, count, align):
        return self.part.at[k, pl.ds(pl.multiple_of(start, align), count), :]

    def c_core(self, k):
        return self.copy(0, k, self.rows(k, self.other, 256, 256), self.r0.at[lax.rem(k, SLOTS)], self.core_peer)

    def c_side(self, k):
        slot = lax.rem(k, SLOTS)
        return (self.copy(1, k, self.rows(k, self.a_far, 64, 64), self.r1.at[slot, pl.ds(0, 64), :], self.x_peer),
                self.copy(2, k, self.rows(k, self.b_far, 64, 64), self.r1.at[slot, pl.ds(64, 64), :], self.y_peer))

    def c_in(self, k):
        slot = lax.rem(k, SLOTS)
        return (self.copy(3, k, self.rows(k, self.a, 64, 64), self.r2.at[slot, pl.ds(0, 64), :], self.z_inner),
                self.copy(4, k, self.rows(k, self.b, 64, 64), self.r2.at[slot, pl.ds(64, 64), :], self.z_inner))

    def c_pair(self, k):
        slot, far = lax.rem(k, SLOTS), (1 - self.mid) * 32
        return (self.copy(5, k, self.rows(k, self.a + far, 32, 32), self.r3.at[slot, pl.ds(0, 32), :], self.z_peer),
                self.copy(6, k, self.rows(k, self.b + far, 32, 32), self.r3.at[slot, pl.ds(32, 32), :], self.z_peer))

    def c_turn(self, k):
        slot, near = lax.rem(k, SLOTS), self.mid * 32
        return (self.copy(7, k, self.rows(k, self.a + near, 32, 32), self.r4.at[slot, pl.ds(0, 32), :], self.y_peer),
                self.copy(8, k, self.rows(k, self.b + near, 32, 32), self.r4.at[slot, pl.ds(32, 32), :], self.x_peer))

    def c_back(self, k):
        near = self.mid * 32
        a, b = self.rows(k, self.a + near, 32, 32), self.rows(k, self.b + near, 32, 32)
        return (self.copy(9, k, a, a, self.z_peer), self.copy(10, k, b, b, self.z_peer))

    def c_out(self, k, kind, at):
        a, b = self.rows(k, self.a + at, 32, 32), self.rows(k, self.b + at, 32, 32)
        return (self.copy(kind, k, a, a, self.z_outer), self.copy(kind + 1, k, b, b, self.z_outer))

    def c_wide(self, k):
        a, b = self.rows(k, self.a, 64, 64), self.rows(k, self.b, 64, 64)
        return (self.copy(15, k, a, a, self.x_peer), self.copy(16, k, b, b, self.y_peer))

    def c_full(self, k):
        half = self.rows(k, self.own, 256, 256)
        return self.copy(17, k, half, half, self.core_peer)

    def release(self, kind, peer):
        pl.semaphore_signal(self.free.at[kind], inc=1, device_id=peer, device_id_type=MESH)

    def stage(self, s, k):
        part, slot = self.part.at[k], lax.rem(k, SLOTS)
        if s == 0:
            self.ready(k)
            self.c_core(k).start()
        elif s == 1:
            self.c_core(k).wait()
            self.release(0, self.core_peer)
            r0 = self.r0.at[slot]
            add_rows(part, self.own, r0, 0, 256)
            for c in self.c_side(k):
                c.start()
        elif s == 2:
            for c in self.c_side(k):
                c.wait()
            add_rows(part, self.a, self.r1.at[slot], 0, 64)
            add_rows(part, self.b, self.r1.at[slot], 64, 64)

            @pl.when(self.outer)
            def _():
                for c in self.c_in(k):
                    c.start()
        elif s == 3:
            @pl.when(self.inner)
            def _():
                for c in self.c_in(k):
                    c.wait_recv()
                add_rows(part, self.a, self.r2.at[slot], 0, 64)
                add_rows(part, self.b, self.r2.at[slot], 64, 64)
                for c in self.c_pair(k):
                    c.start()

            @pl.when(self.outer)
            def _():
                for c in self.c_in(k):
                    c.wait_send()
                self.release(1, self.z_inner)
        elif s == 4:
            @pl.when(self.inner)
            def _():
                for c in self.c_pair(k):
                    c.wait()
                self.release(2, self.z_peer)
                add_rows(part, self.a + self.mid * 32, self.r3.at[slot], 0, 32)
                add_rows(part, self.b + self.mid * 32, self.r3.at[slot], 32, 32)
                for c in self.c_turn(k):
                    c.start()
        elif s == 5:
            @pl.when(self.inner)
            def _():
                for c in self.c_turn(k):
                    c.wait()
                add_rows(part, self.a + self.mid * 32, self.r4.at[slot], 0, 32, self.scale)
                add_rows(part, self.b + self.mid * 32, self.r4.at[slot], 32, 32, self.scale)
                pl.semaphore_wait(self.free.at[1], 1)
                pl.semaphore_wait(self.free.at[2], 1)
                for c in self.c_back(k) + self.c_out(k, 11, self.mid * 32):
                    c.start()
        elif s == 6:
            @pl.when(self.inner)
            def _():
                for c in self.c_back(k):
                    c.wait_recv()
                for c in self.c_out(k, 13, (1 - self.mid) * 32) + self.c_wide(k):
                    c.start()
        elif s == 7:
            @pl.when(self.outer)
            def _():
                for c in self.c_out(k, 11, 0) + self.c_out(k, 13, 0):
                    c.wait_recv()
                for c in self.c_wide(k):
                    c.start()
        elif s == 8:
            for c in self.c_wide(k):
                c.wait_recv()
            pl.semaphore_wait(self.free.at[0], 1)
            self.c_full(k).start()
        elif s == 9:
            self.c_full(k).wait_recv()
            self.emit(k)

    def tick(self, t):
        for s in reversed(range(STAGES)):
            k = t - LAG[s]

            @pl.when((k >= 0) & (k < self.total))
            def _():
                self.stage(s, k)

    def drain(self):
        def body(k, _):
            for c in self.c_wide(k):
                c.wait_send()
            self.c_full(k).wait_send()

            @pl.when(self.inner)
            def _():
                for c in self.c_back(k) + self.c_out(k, 11, 0) + self.c_out(k, 13, 0):
                    c.wait_send()
            return 0

        lax.fori_loop(0, self.total, body, 0)


def reduce_kernel(groups, scale, *refs):
    n = len(groups)
    ins, outs = refs[:n], refs[n:2 * n]
    part, r0, r1, r2, r3, r4, send, recv, free, load_sem, store_sem = refs[2 * n:]
    total = sum(len(blocks_of(g)) for g in groups)

    k = 0
    for ref, shape in zip(ins, groups):
        for r, c in blocks_of(shape):
            pltpu.make_async_copy(ref.at[pl.ds(r, SIDE), pl.ds(c, SIDE)], part.at[k], load_sem.at[k]).start()
            k += 1

    def ready(k):
        pltpu.make_async_copy(ins[0].at[pl.ds(0, SIDE), pl.ds(0, SIDE)], part.at[k], load_sem.at[k]).wait()

    def emit(k):
        first = 0
        for ref, shape in zip(outs, groups):
            count = len(blocks_of(shape))
            base = first

            @pl.when((k >= base) & (k < base + count))
            def _():
                at = pl.multiple_of((k - base) * SIDE, SIDE)
                dst = ref.at[pl.ds(at, SIDE), :] if shape[1] == SIDE else ref.at[:, pl.ds(at, SIDE)]
                pltpu.make_async_copy(part.at[k], dst, store_sem.at[k]).start()
            first += count

    ex = Exchange(total, scale, part, r0, r1, r2, r3, r4, send, recv, free, ready, emit)
    ex.barrier()

    def step(t, _):
        ex.tick(t)
        return 0

    lax.fori_loop(0, total + LAG[-1], step, 0)
    ex.drain()

    def stored(k, _):
        pltpu.make_async_copy(part.at[k], outs[0].at[pl.ds(0, SIDE), pl.ds(0, SIDE)], store_sem.at[k]).wait()
        return 0

    lax.fori_loop(0, total, stored, 0)


def all_mean(grads, scale):
    groups = tuple(g.shape for g in grads)
    total = sum(len(blocks_of(g)) for g in groups)
    any_spec = pl.BlockSpec(memory_space=pl.ANY)
    return pl.pallas_call(
        functools.partial(reduce_kernel, groups, scale),
        out_shape=[jax.ShapeDtypeStruct(g.shape, F32) for g in grads],
        in_specs=[any_spec] * len(grads),
        out_specs=[any_spec] * len(grads),
        scratch_shapes=[
            pltpu.VMEM((total, SIDE, SIDE), F32),
            pltpu.VMEM((SLOTS, 256, SIDE), F32),
            pltpu.VMEM((SLOTS, 128, SIDE), F32),
            pltpu.VMEM((SLOTS, 128, SIDE), F32),
            pltpu.VMEM((SLOTS, 64, SIDE), F32),
            pltpu.VMEM((SLOTS, 64, SIDE), F32),
            pltpu.SemaphoreType.DMA((18, total)),
            pltpu.SemaphoreType.DMA((18, total)),
            pltpu.SemaphoreType.REGULAR((3,)),
            pltpu.SemaphoreType.DMA((total,)),
            pltpu.SemaphoreType.DMA((total,)),
        ],
        compiler_params=pltpu.CompilerParams(
            collective_id=0, has_side_effects=True, vmem_limit_bytes=66 * 1000 * 1000),
        name="mean_over_devices",
    )(*grads)


def solution(mesh):
    batch_axes = ("z", "y", "x")
    scale = 1.0 / mesh.size
    row_spec = P(batch_axes, None)
    full_spec = P(None, None)

    def device_step(x_in, g_out, w_in, w_up1, w_down1, w_up2, w_down2):
        x_mid = plain_product(x_in, w_in).astype(jnp.bfloat16)
        pre_one = plain_product(x_mid, w_up1).astype(jnp.bfloat16)
        act_one = gelu_value(pre_one).astype(jnp.bfloat16)
        hid_two = (plain_product(act_one, w_down1) + x_mid.astype(jnp.float32)).astype(jnp.bfloat16)
        pre_three = plain_product(hid_two, w_up2).astype(jnp.bfloat16)
        act_three = gelu_value(pre_three).astype(jnp.bfloat16)
        dw_down2 = rows_contract(act_three, g_out)
        d_act3 = times_transposed(g_out, w_down2).astype(jnp.bfloat16)
        d_pre3 = (d_act3.astype(jnp.float32) * gelu_slope(pre_three)).astype(jnp.bfloat16)
        dw_up2 = rows_contract(hid_two, d_pre3)
        d_hid2 = (times_transposed(d_pre3, w_up2) + g_out.astype(jnp.float32)).astype(jnp.bfloat16)
        dw_down1 = rows_contract(act_one, d_hid2)
        d_act1 = times_transposed(d_hid2, w_down1).astype(jnp.bfloat16)
        d_pre1 = (d_act1.astype(jnp.float32) * gelu_slope(pre_one)).astype(jnp.bfloat16)
        dw_up1 = rows_contract(x_mid, d_pre1)
        d_mid = (times_transposed(d_pre1, w_up1) + d_hid2.astype(jnp.float32)).astype(jnp.bfloat16)
        dw_in = rows_contract(x_in, d_mid)
        dx_rows = times_transposed(d_mid, w_in).astype(jnp.bfloat16)
        dw_down2, dw_up2, dw_down1, dw_up1, dw_in = all_mean([dw_down2, dw_up2, dw_down1, dw_up1, dw_in], scale)
        return dx_rows, dw_in, dw_up1, dw_down1, dw_up2, dw_down2

    return jax.shard_map(
        device_step,
        mesh=mesh,
        in_specs=(row_spec, row_spec, full_spec, full_spec, full_spec, full_spec, full_spec),
        out_specs=(row_spec, full_spec, full_spec, full_spec, full_spec, full_spec),
        check_vma=False,
    )
```

```python
import functools
import jax
import jax.numpy as jnp
from jax import lax
from jax.experimental import pallas as pl
from jax.experimental.pallas import tpu as pltpu
from jax.sharding import PartitionSpec as P

SQRT_HALF = 0.7071067811865476
INV_SQRT_TAU = 0.3989422804014327
MESH = pl.DeviceIdType.MESH
F32 = jnp.float32
BF16 = jnp.bfloat16

SIDE = 512
SLOTS = 8
STAGES = 10
LAG = (0, 1, 2, 3, 4, 5, 6, 7, 8, 9)


def gelu_value(pre_act):
    pre_wide = pre_act.astype(jnp.float32)
    return 0.5 * pre_wide * (1.0 + lax.erf(pre_wide * SQRT_HALF))


def gelu_slope(pre_act):
    pre_wide = pre_act.astype(jnp.float32)
    return 0.5 * (1.0 + lax.erf(pre_wide * SQRT_HALF)) + pre_wide * jnp.exp(-0.5 * pre_wide * pre_wide) * INV_SQRT_TAU


def plain_product(first_op, second_op):
    return lax.dot_general(first_op, second_op, (((1,), (0,)), ((), ())), preferred_element_type=jnp.float32)


def rows_contract(first_op, second_op):
    return lax.dot_general(first_op, second_op, (((0,), (0,)), ((), ())), preferred_element_type=jnp.float32)


def times_transposed(first_op, second_op):
    return lax.dot_general(first_op, second_op, (((1,), (1,)), ((), ())), preferred_element_type=jnp.float32)


def blocks_of(shape):
    rows, cols = shape
    return [(r, c) for r in range(0, rows, SIDE) for c in range(0, cols, SIDE)]


def add_rows(dst, dst_row, src, src_row, count, scale=None):
    step = 16

    def body(i, _):
        at = pl.ds(pl.multiple_of(dst_row + i * step, step), step)
        value = dst[at, :] + src[pl.ds(pl.multiple_of(src_row + i * step, step), step), :]
        dst[at, :] = value if scale is None else value * scale
        return 0

    lax.fori_loop(0, count // step, body, 0, unroll=True)


class Exchange:
    def __init__(self, total, scale, part, r0, r1, r2, r3, r4, send, recv, free, ready, emit):
        self.free = free
        self.total, self.scale, self.part = total, scale, part
        self.r0, self.r1, self.r2, self.r3, self.r4 = r0, r1, r2, r3, r4
        self.send, self.recv, self.ready, self.emit = send, recv, ready, emit
        z, y, x = lax.axis_index("z"), lax.axis_index("y"), lax.axis_index("x")
        core, chip = lax.rem(x, 2), x // 2
        self.z = z
        self.core_peer = (z, y, chip * 2 + 1 - core)
        self.x_peer = (z, y, (1 - chip) * 2 + core)
        self.y_peer = (z, 1 - y, x)
        self.inner = (z >= 1) & (z <= 2)
        self.outer = (z == 0) | (z == 3)
        self.mid = jnp.where(z >= 2, 1, 0)
        self.z_inner = (jnp.where(z == 0, 1, 2), y, x)
        self.z_peer = (jnp.where(z == 1, 2, 1), y, x)
        self.z_outer = (jnp.where(z == 1, 0, 3), y, x)
        half = SIDE // 2
        self.own = core * half
        self.other = (1 - core) * half
        self.a = self.own + chip * (half // 4)
        self.a_far = self.own + (1 - chip) * (half // 4)
        self.b = self.own + half // 2 + y * (half // 4)
        self.b_far = self.own + half // 2 + (1 - y) * (half // 4)

    def barrier(self):
        sem = pltpu.get_barrier_semaphore()
        for peer in (self.core_peer, self.x_peer, self.y_peer):
            pl.semaphore_signal(sem, inc=1, device_id=peer, device_id_type=MESH)

        @pl.when(self.inner)
        def _():
            pl.semaphore_signal(sem, inc=1, device_id=self.z_peer, device_id_type=MESH)
            pl.semaphore_signal(sem, inc=1, device_id=self.z_outer, device_id_type=MESH)
            pl.semaphore_wait(sem, 5)

        @pl.when(self.outer)
        def _():
            pl.semaphore_signal(sem, inc=1, device_id=self.z_inner, device_id_type=MESH)
            pl.semaphore_wait(sem, 4)

    def copy(self, kind, k, src, dst, peer):
        return pltpu.make_async_remote_copy(
            src_ref=src, dst_ref=dst, send_sem=self.send.at[kind, k], recv_sem=self.recv.at[kind, k],
            device_id=peer, device_id_type=MESH)

    def rows(self, k, start, count, align):
        return self.part.at[k, pl.ds(pl.multiple_of(start, align), count), :]

    def c_core(self, k):
        return self.copy(0, k, self.rows(k, self.other, 256, 256), self.r0.at[lax.rem(k, SLOTS)], self.core_peer)

    def c_side(self, k):
        slot = lax.rem(k, SLOTS)
        return (self.copy(1, k, self.rows(k, self.a_far, 64, 64), self.r1.at[slot, pl.ds(0, 64), :], self.x_peer),
                self.copy(2, k, self.rows(k, self.b_far, 64, 64), self.r1.at[slot, pl.ds(64, 64), :], self.y_peer))

    def c_in(self, k):
        slot = lax.rem(k, SLOTS)
        return (self.copy(3, k, self.rows(k, self.a, 64, 64), self.r2.at[slot, pl.ds(0, 64), :], self.z_inner),
                self.copy(4, k, self.rows(k, self.b, 64, 64), self.r2.at[slot, pl.ds(64, 64), :], self.z_inner))

    def c_pair(self, k):
        slot, far = lax.rem(k, SLOTS), (1 - self.mid) * 32
        return (self.copy(5, k, self.rows(k, self.a + far, 32, 32), self.r3.at[slot, pl.ds(0, 32), :], self.z_peer),
                self.copy(6, k, self.rows(k, self.b + far, 32, 32), self.r3.at[slot, pl.ds(32, 32), :], self.z_peer))

    def c_turn(self, k):
        slot, near = lax.rem(k, SLOTS), self.mid * 32
        return (self.copy(7, k, self.rows(k, self.a + near, 32, 32), self.r4.at[slot, pl.ds(0, 32), :], self.y_peer),
                self.copy(8, k, self.rows(k, self.b + near, 32, 32), self.r4.at[slot, pl.ds(32, 32), :], self.x_peer))

    def c_back(self, k):
        near = self.mid * 32
        a, b = self.rows(k, self.a + near, 32, 32), self.rows(k, self.b + near, 32, 32)
        return (self.copy(9, k, a, a, self.z_peer), self.copy(10, k, b, b, self.z_peer))

    def c_out(self, k, kind, at):
        a, b = self.rows(k, self.a + at, 32, 32), self.rows(k, self.b + at, 32, 32)
        return (self.copy(kind, k, a, a, self.z_outer), self.copy(kind + 1, k, b, b, self.z_outer))

    def c_wide(self, k):
        a, b = self.rows(k, self.a, 64, 64), self.rows(k, self.b, 64, 64)
        return (self.copy(15, k, a, a, self.x_peer), self.copy(16, k, b, b, self.y_peer))

    def c_full(self, k):
        half = self.rows(k, self.own, 256, 256)
        return self.copy(17, k, half, half, self.core_peer)

    def release(self, kind, peer):
        pl.semaphore_signal(self.free.at[kind], inc=1, device_id=peer, device_id_type=MESH)

    def stage(self, s, k):
        part, slot = self.part.at[k], lax.rem(k, SLOTS)
        if s == 0:
            self.ready(k)
            self.c_core(k).start()
        elif s == 1:
            self.c_core(k).wait()
            self.release(0, self.core_peer)
            r0 = self.r0.at[slot]
            add_rows(part, self.own, r0, 0, 256)
            for c in self.c_side(k):
                c.start()
        elif s == 2:
            for c in self.c_side(k):
                c.wait()
            add_rows(part, self.a, self.r1.at[slot], 0, 64)
            add_rows(part, self.b, self.r1.at[slot], 64, 64)

            @pl.when(self.outer)
            def _():
                for c in self.c_in(k):
                    c.start()
        elif s == 3:
            @pl.when(self.inner)
            def _():
                for c in self.c_in(k):
                    c.wait_recv()
                add_rows(part, self.a, self.r2.at[slot], 0, 64)
                add_rows(part, self.b, self.r2.at[slot], 64, 64)
                for c in self.c_pair(k):
                    c.start()

            @pl.when(self.outer)
            def _():
                for c in self.c_in(k):
                    c.wait_send()
                self.release(1, self.z_inner)
        elif s == 4:
            @pl.when(self.inner)
            def _():
                for c in self.c_pair(k):
                    c.wait()
                self.release(2, self.z_peer)
                add_rows(part, self.a + self.mid * 32, self.r3.at[slot], 0, 32)
                add_rows(part, self.b + self.mid * 32, self.r3.at[slot], 32, 32)
                for c in self.c_turn(k):
                    c.start()
        elif s == 5:
            @pl.when(self.inner)
            def _():
                for c in self.c_turn(k):
                    c.wait()
                add_rows(part, self.a + self.mid * 32, self.r4.at[slot], 0, 32, self.scale)
                add_rows(part, self.b + self.mid * 32, self.r4.at[slot], 32, 32, self.scale)
                pl.semaphore_wait(self.free.at[1], 1)
                pl.semaphore_wait(self.free.at[2], 1)
                for c in self.c_back(k) + self.c_out(k, 11, self.mid * 32):
                    c.start()
        elif s == 6:
            @pl.when(self.inner)
            def _():
                for c in self.c_back(k):
                    c.wait_recv()
                for c in self.c_out(k, 13, (1 - self.mid) * 32) + self.c_wide(k):
                    c.start()
        elif s == 7:
            @pl.when(self.outer)
            def _():
                for c in self.c_out(k, 11, 0) + self.c_out(k, 13, 0):
                    c.wait_recv()
                for c in self.c_wide(k):
                    c.start()
        elif s == 8:
            for c in self.c_wide(k):
                c.wait_recv()
            pl.semaphore_wait(self.free.at[0], 1)
            self.c_full(k).start()
        elif s == 9:
            self.c_full(k).wait_recv()
            self.emit(k)

    def tick(self, t):
        for s in reversed(range(STAGES)):
            k = t - LAG[s]

            @pl.when((k >= 0) & (k < self.total))
            def _():
                self.stage(s, k)

    def drain(self):
        def body(k, _):
            for c in self.c_wide(k):
                c.wait_send()
            self.c_full(k).wait_send()

            @pl.when(self.inner)
            def _():
                for c in self.c_back(k) + self.c_out(k, 11, 0) + self.c_out(k, 13, 0):
                    c.wait_send()
            return 0

        lax.fori_loop(0, self.total, body, 0)


def backward_kernel(groups, scale, *refs):
    (dw4, g_in, a3, h2, a1, h1, m_in, x0, w4, w3, w2, w1), refs = refs[:12], refs[12:]
    outs, dm_out, refs = refs[:5], refs[5], refs[6:]
    part, r0, r1, r2, r3, r4, d_act, w_down, w_up, g_buf, lhs, dh2, col = refs[:13]
    send, recv, free, load_sem, store_sem, side_sem, col_sem = refs[13:]
    total = sum(len(blocks_of(g)) for g in groups)

    def load(n, src, dst):
        return pltpu.make_async_copy(src, dst, side_sem.at[n])

    streams = ((a3, 0, 4), (h1, 4, 4), (a1, 8, 4), (x0, 12, 8))

    def fetch(n):
        for ref, first, count in streams:
            @pl.when((n >= first) & (n < first + count))
            def _():
                at = pl.ds(pl.multiple_of((n - first) * SIDE, SIDE), SIDE)
                slot = lax.rem(n, 2)
                pltpu.make_async_copy(ref.at[:, at], col.at[slot], col_sem.at[slot]).start()

    def fetched(n):
        slot = lax.rem(n, 2)
        pltpu.make_async_copy(a3.at[:, pl.ds(0, SIDE)], col.at[slot], col_sem.at[slot]).wait()
        return col.at[slot]

    load(0, g_in, g_buf).start()
    load(1, w4, w_down).start()
    fetch(0)
    load(2, h2, lhs).start()
    fetch(1)
    load(3, w3, w_up).start()
    for k in range(4):
        pltpu.make_async_copy(dw4.at[pl.ds(k * SIDE, SIDE), :], part.at[k], load_sem.at[k]).start()

    def ready(k):
        @pl.when(k < 4)
        def _():
            pltpu.make_async_copy(dw4.at[pl.ds(0, SIDE), :], part.at[k], load_sem.at[k]).wait()

    def emit(k):
        first = 0
        for ref, shape in zip(outs, groups):
            count = len(blocks_of(shape))
            base = first

            @pl.when((k >= base) & (k < base + count))
            def _():
                at = pl.multiple_of((k - base) * SIDE, SIDE)
                dst = ref.at[pl.ds(at, SIDE), :] if shape[1] == SIDE else ref.at[:, pl.ds(at, SIDE)]
                pltpu.make_async_copy(part.at[k], dst, store_sem.at[k]).start()
            first += count

    def grad_block(k, left, right, right_cols):
        for piece in range(2):
            rows = pl.ds(piece * 1024, 1024)
            value = rows_contract(left[rows, :], right[rows, right_cols])
            if piece == 0:
                part[k] = value
            else:
                part[k] += value

    def slope_block(j, grad, act):
        at = pl.ds(pl.multiple_of(j * SIDE, SIDE), SIDE)

        def body(t, _):
            rows = pl.ds(pl.multiple_of(t * 256, 256), 256)
            d_out = times_transposed(grad[rows, :], w_down[at, :]).astype(BF16)
            d_act[rows, at] = (d_out.astype(F32) * gelu_slope(act[rows, :])).astype(BF16)
            return 0

        lax.fori_loop(0, 8, body, 0)
        return at

    def back_rows(add, dst):
        def body(t, _):
            rows = pl.ds(pl.multiple_of(t * 512, 512), 512)
            dst[rows, :] = (times_transposed(d_act[rows, :], w_up[...]) + add[rows, :].astype(F32)).astype(BF16)
            return 0

        lax.fori_loop(0, 4, body, 0)

    def compute(i):
        @pl.when(i == 1)
        def _():
            load(0, g_in, g_buf).wait()
            load(1, w4, w_down).wait()
            load(2, h2, lhs).wait()

        @pl.when(i == 8)
        def _():
            load(4, w2, w_down).wait()
            load(5, m_in, lhs).wait()

        for first, n0, grad, k0 in ((1, 0, g_buf, 4), (8, 8, dh2, 12)):
            @pl.when((i >= first) & (i < first + 4))
            def _():
                j = i - first
                act = fetched(n0 + j)
                at = slope_block(j, grad, act)
                fetch(n0 + j + 2)
                grad_block(k0 + j, lhs, d_act, at)

        @pl.when(i == 4)
        def _():
            load(4, w2, w_down).start()
            load(5, m_in, lhs).start()

        @pl.when(i == 5)
        def _():
            load(3, w3, w_up).wait()
            back_rows(g_buf, dh2)
            load(6, w1, w_up).start()

        @pl.when(i == 12)
        def _():
            load(6, w1, w_up).wait()
            back_rows(dh2, g_buf)
            load(7, g_buf, dm_out).start()

        for first, count, n0, right, k0 in ((6, 2, 4, dh2, 8), (13, 4, 12, g_buf, 16)):
            @pl.when((i >= first) & (i < first + count))
            def _():
                def body(e, _):
                    j = (i - first) * 2 + e
                    left = fetched(n0 + j)
                    grad_block(k0 + j, left, right, slice(None))
                    fetch(n0 + j + 2)
                    return 0

                lax.fori_loop(0, 2, body, 0)

    ex = Exchange(total, scale, part, r0, r1, r2, r3, r4, send, recv, free, ready, emit)
    ex.barrier()

    def step(i, _):
        compute(i)
        ex.tick(i)
        return 0

    lax.fori_loop(0, total + LAG[-1], step, 0)
    ex.drain()
    load(7, g_buf, dm_out).wait()

    def stored(k, _):
        pltpu.make_async_copy(part.at[k], outs[0].at[pl.ds(0, SIDE), pl.ds(0, SIDE)], store_sem.at[k]).wait()
        return 0

    lax.fori_loop(0, total, stored, 0)


def backward(dw4, g, a3, h2, a1, h1, m, x0, w4, w3, w2, w1, groups, scale):
    total = sum(len(blocks_of(g)) for g in groups)
    any_spec = pl.BlockSpec(memory_space=pl.ANY)
    rows, wide = a3.shape
    return pl.pallas_call(
        functools.partial(backward_kernel, groups, scale),
        out_shape=[jax.ShapeDtypeStruct(g, F32) for g in groups] + [jax.ShapeDtypeStruct((rows, SIDE), BF16)],
        in_specs=[any_spec] * 12,
        out_specs=[any_spec] * 6,
        scratch_shapes=[
            pltpu.VMEM((total, SIDE, SIDE), F32),
            pltpu.VMEM((SLOTS, 256, SIDE), F32),
            pltpu.VMEM((SLOTS, 128, SIDE), F32),
            pltpu.VMEM((SLOTS, 128, SIDE), F32),
            pltpu.VMEM((SLOTS, 64, SIDE), F32),
            pltpu.VMEM((SLOTS, 64, SIDE), F32),
            pltpu.VMEM((rows, wide), BF16),
            pltpu.VMEM((wide, SIDE), BF16),
            pltpu.VMEM((SIDE, wide), BF16),
            pltpu.VMEM((rows, SIDE), BF16),
            pltpu.VMEM((rows, SIDE), BF16),
            pltpu.VMEM((rows, SIDE), BF16),
            pltpu.VMEM((2, rows, SIDE), BF16),
            pltpu.SemaphoreType.DMA((18, total)),
            pltpu.SemaphoreType.DMA((18, total)),
            pltpu.SemaphoreType.REGULAR((3,)),
            pltpu.SemaphoreType.DMA((4,)),
            pltpu.SemaphoreType.DMA((total,)),
            pltpu.SemaphoreType.DMA((8,)),
            pltpu.SemaphoreType.DMA((2,)),
        ],
        compiler_params=pltpu.CompilerParams(
            collective_id=0, has_side_effects=True, vmem_limit_bytes=67 * 1000 * 1000),
        name="backward_and_mean",
    )(dw4, g, a3, h2, a1, h1, m, x0, w4, w3, w2, w1)


def finish_kernel(groups, dm, w0, *refs):
    ins, dx, outs = refs[:5], refs[5], refs[6:11]
    through, rows_out, in_sem, out_sem, dx_sem = refs[11:]
    moves = [(src, dst, r) for src, dst, shape in zip(ins, outs, groups) for r in range(0, shape[0], 128 if shape[1] > SIDE else SIDE)]
    depth = 6

    def views(n):
        src, dst, r = moves[n]
        count = 128 if src.shape[1] > SIDE else SIDE
        buf = through[0] if src.shape[1] == SIDE else through[1]
        return src.at[pl.ds(r, count), :], buf.at[n % depth], dst.at[pl.ds(r, count), :]

    def start_in(n):
        src, mid, _ = views(n)
        pltpu.make_async_copy(src, mid, in_sem.at[n]).start()

    def pass_on(n):
        src, mid, dst = views(n)
        pltpu.make_async_copy(src, mid, in_sem.at[n]).wait()
        pltpu.make_async_copy(mid, dst, out_sem.at[n]).start()

    def passed(n):
        _, mid, dst = views(n)
        pltpu.make_async_copy(mid, dst, out_sem.at[n]).wait()

    def dx_copy(i):
        return pltpu.make_async_copy(rows_out.at[i % 2], dx.at[pl.ds(i * 128, 128), :], dx_sem.at[i % 2])

    for n in range(depth // 2):
        start_in(n)
    steps, width = 16, 4096
    done = 0
    for i in range(steps):
        for n in range(done, (i + 1) * len(moves) // steps):
            if n + depth // 2 < len(moves):
                if n - depth // 2 >= 0:
                    passed(n - depth // 2)
                start_in(n + depth // 2)
            pass_on(n)
            done = n + 1
        if i >= 2:
            dx_copy(i - 2).wait()

        def column(j, _):
            at = pl.ds(pl.multiple_of(j * 1024, 1024), 1024)
            rows_out[i % 2, :, at] = times_transposed(dm[pl.ds(i * 128, 128), :], w0[at, :]).astype(BF16)
            return 0

        lax.fori_loop(0, width // 1024, column, 0)
        dx_copy(i).start()
    for i in (steps - 2, steps - 1):
        dx_copy(i).wait()
    for n in range(max(0, len(moves) - depth), len(moves)):
        passed(n)


def solution(mesh):
    batch_axes = ("z", "y", "x")
    scale = 1.0 / mesh.size
    row_spec = P(batch_axes, None)
    full_spec = P(None, None)

    def device_step(x_in, g_out, w_in, w_up1, w_down1, w_up2, w_down2):
        x_mid = plain_product(x_in, w_in).astype(jnp.bfloat16)
        pre_one = plain_product(x_mid, w_up1).astype(jnp.bfloat16)
        act_one = gelu_value(pre_one).astype(jnp.bfloat16)
        hid_two = (plain_product(act_one, w_down1) + x_mid.astype(jnp.float32)).astype(jnp.bfloat16)
        pre_three = plain_product(hid_two, w_up2).astype(jnp.bfloat16)
        act_three = gelu_value(pre_three).astype(jnp.bfloat16)
        dw_down2 = rows_contract(act_three, g_out)
        groups = (dw_down2.shape, w_up2.shape, w_down1.shape, w_up1.shape, w_in.shape)
        dw_down2, dw_up2, dw_down1, dw_up1, dw_in, d_mid = backward(
            dw_down2, g_out, pre_three, hid_two, pre_one, act_one, x_mid, x_in, w_down2, w_up2, w_down1, w_up1, groups, scale)
        dx_rows = times_transposed(d_mid, w_in).astype(jnp.bfloat16)
        return dx_rows, dw_in, dw_up1, dw_down1, dw_up2, dw_down2

    return jax.shard_map(
        device_step,
        mesh=mesh,
        in_specs=(row_spec, row_spec, full_spec, full_spec, full_spec, full_spec, full_spec),
        out_specs=(row_spec, full_spec, full_spec, full_spec, full_spec, full_spec),
        check_vma=False,
    )
```

```python
import functools
import jax
import jax.numpy as jnp
from jax import lax
from jax.experimental import pallas as pl
from jax.experimental.pallas import tpu as pltpu
from jax.sharding import PartitionSpec as P

SQRT_HALF = 0.7071067811865476
INV_SQRT_TAU = 0.3989422804014327
MESH = pl.DeviceIdType.MESH
F32 = jnp.float32
BF16 = jnp.bfloat16

SIDE = 512
UNIT = SIDE // 2
SLOTS = 8
TURNS = 16
LAG = (0, 2, 4, 6, 8, 10, 12, 14, 16, 18, 20, 22)


def gelu_value(pre_act):
    pre_wide = pre_act.astype(jnp.float32)
    return 0.5 * pre_wide * (1.0 + lax.erf(pre_wide * SQRT_HALF))


def gelu_slope(pre_act):
    pre_wide = pre_act.astype(jnp.float32)
    return 0.5 * (1.0 + lax.erf(pre_wide * SQRT_HALF)) + pre_wide * jnp.exp(-0.5 * pre_wide * pre_wide) * INV_SQRT_TAU


def plain_product(first_op, second_op):
    return lax.dot_general(first_op, second_op, (((1,), (0,)), ((), ())), preferred_element_type=jnp.float32)


def rows_contract(first_op, second_op):
    return lax.dot_general(first_op, second_op, (((0,), (0,)), ((), ())), preferred_element_type=jnp.float32)


def times_transposed(first_op, second_op):
    return lax.dot_general(first_op, second_op, (((1,), (1,)), ((), ())), preferred_element_type=jnp.float32)


def blocks_of(shape):
    rows, cols = shape
    return [(r, c) for r in range(0, rows, SIDE) for c in range(0, cols, SIDE)]


class Exchange:
    def __init__(self, total, scale, part, r0, r1, r2, r3, r4, send, recv, free, ready, emit):
        self.total, self.scale, self.part = total, scale, part
        self.r0, self.r1, self.r2, self.r3, self.r4 = r0, r1, r2, r3, r4
        self.send, self.recv, self.free, self.ready, self.emit = send, recv, free, ready, emit
        z, y, x = lax.axis_index("z"), lax.axis_index("y"), lax.axis_index("x")
        core, chip = lax.rem(x, 2), x // 2
        self.core_peer = (z, y, chip * 2 + 1 - core)
        self.x_peer = (z, y, (1 - chip) * 2 + core)
        self.y_peer = (z, 1 - y, x)
        self.inner = (z >= 1) & (z <= 2)
        self.outer = (z == 0) | (z == 3)
        self.z_inner = (jnp.where(z == 0, 1, 2), y, x)
        self.z_peer = (jnp.where(z == 1, 2, 1), y, x)
        self.z_outer = (jnp.where(z == 1, 0, 3), y, x)
        half, self.q = UNIT // 2, UNIT // 8
        n = self.n = self.q // 4
        self.half = half
        self.own = core * half
        self.other = (1 - core) * half
        self.a = self.own + chip * self.q
        self.a_far = self.own + (1 - chip) * self.q
        self.b = self.own + half // 2 + y * self.q
        self.b_far = self.own + half // 2 + (1 - y) * self.q
        high = jnp.where(z >= 2, 1, 0)
        self.to_in = n * (1 - high)
        self.to_pair = 2 * n * (1 - high)
        self.from_pair = 2 * n * high
        self.to_out = 3 * n * high
        self.mine = n * z
        self.twin = n * (3 - z)
        self.far = 3 * n * (1 - high)

    def barrier(self):
        sem = pltpu.get_barrier_semaphore()
        for peer in (self.core_peer, self.x_peer, self.y_peer):
            pl.semaphore_signal(sem, inc=1, device_id=peer, device_id_type=MESH)

        @pl.when(self.inner)
        def _():
            pl.semaphore_signal(sem, inc=1, device_id=self.z_peer, device_id_type=MESH)
            pl.semaphore_signal(sem, inc=1, device_id=self.z_outer, device_id_type=MESH)
            pl.semaphore_wait(sem, 5)

        @pl.when(self.outer)
        def _():
            pl.semaphore_signal(sem, inc=1, device_id=self.z_inner, device_id_type=MESH)
            pl.semaphore_wait(sem, 4)

    def copy(self, kind, k, src, dst, peer):
        turn = lax.rem(k, TURNS)
        return pltpu.make_async_remote_copy(
            src_ref=src, dst_ref=dst, send_sem=self.send.at[kind, turn], recv_sem=self.recv.at[kind, turn],
            device_id=peer, device_id_type=MESH)

    def rows(self, k, start, count):
        at = pl.multiple_of(lax.rem(k, 2) * UNIT + start, 8)
        return self.part.at[k // 2, pl.ds(at, count), :]

    def both(self, kind, k, at, count, peer, into=None):
        slot, out = lax.rem(k, SLOTS), []
        for e, base in enumerate((self.a, self.b)):
            src = self.rows(k, base + at, count)
            dst = src if into is None else into.at[slot, pl.ds(pl.multiple_of(e * self.q + at, 8), count), :]
            out.append(self.copy(kind + e, k, src, dst, peer))
        return out

    def c_core(self, k):
        return [self.copy(0, k, self.rows(k, self.other, self.half), self.r0.at[lax.rem(k, SLOTS)], self.core_peer)]

    def c_side(self, k):
        slot = lax.rem(k, SLOTS)
        return [self.copy(1, k, self.rows(k, self.a_far, self.q), self.r1.at[slot, pl.ds(0, self.q), :], self.x_peer),
                self.copy(2, k, self.rows(k, self.b_far, self.q), self.r1.at[slot, pl.ds(self.q, self.q), :], self.y_peer)]

    def c_in(self, k):
        return self.both(3, k, self.to_in, 3 * self.n, self.z_inner, self.r2)

    def c_pair(self, k):
        return self.both(5, k, self.to_pair, 2 * self.n, self.z_peer, self.r3)

    def c_end(self, k):
        return self.both(7, k, self.to_out, self.n, self.z_outer, self.r2)

    def c_turn(self, k):
        slot, n = lax.rem(k, SLOTS), self.n
        return [self.copy(9, k, self.rows(k, self.a + self.mine, n), self.r4.at[slot, pl.ds(0, n), :], self.y_peer),
                self.copy(10, k, self.rows(k, self.b + self.mine, n), self.r4.at[slot, pl.ds(n, n), :], self.x_peer)]

    def c_mine_pair(self, k):
        return self.both(13, k, self.mine, self.n, self.z_peer)

    def c_mine_out(self, k):
        return self.both(15, k, self.mine, self.n, self.z_outer)

    def c_twin_out(self, k):
        return self.both(17, k, self.twin, self.n, self.z_outer)

    def c_mine_in(self, k):
        return self.both(11, k, self.mine, self.n, self.z_inner)

    def c_end_pair(self, k):
        return self.both(19, k, self.to_out, self.n, self.z_peer)

    def c_far_out(self, k):
        return self.both(21, k, self.far, self.n, self.z_outer)

    def c_wide(self, k):
        a, b = self.rows(k, self.a, self.q), self.rows(k, self.b, self.q)
        return [self.copy(23, k, a, a, self.x_peer), self.copy(24, k, b, b, self.y_peer)]

    def c_full(self, k):
        half = self.rows(k, self.own, self.half)
        return [self.copy(25, k, half, half, self.core_peer)]

    def go(self, make, k):
        for c in make(k):
            c.start()

    def go_lazy(self, make, k):
        @pl.when(k >= TURNS)
        def _():
            for c in make(k - TURNS):
                c.wait_send()

        self.go(make, k)

    def got(self, make, k):
        for c in make(k):
            c.wait_recv()

    def sent(self, make, k):
        for c in make(k):
            c.wait_send()

    def release(self, kind, peer):
        pl.semaphore_signal(self.free.at[kind], inc=1, device_id=peer, device_id_type=MESH)

    def add(self, k, at, src, src_row, count, scale=None):
        base = lax.rem(k, 2) * UNIT + at
        block = k // 2
        step = 16 if count % 16 == 0 else 8
        for i in range(0, count, step):
            rows = pl.ds(pl.multiple_of(base + i, 8), step)
            value = self.part[block, rows, :] + src[pl.ds(pl.multiple_of(src_row + i, 8), step), :]
            self.part[block, rows, :] = value if scale is None else value * scale

    def add_both(self, k, at, src, count):
        for e, base in enumerate((self.a, self.b)):
            self.add(k, base + at, src, e * self.q + at, count)

    def turn_done(self, k, r4):
        for c in self.c_turn(k):
            c.wait()
        self.add(k, self.a + self.mine, r4, 0, self.n, self.scale)
        self.add(k, self.b + self.mine, r4, self.n, self.n, self.scale)

    def stage(self, s, k):
        slot = lax.rem(k, SLOTS)
        r0, r1, r2, r3, r4 = (r.at[slot] for r in (self.r0, self.r1, self.r2, self.r3, self.r4))

        def on_inner(f):
            pl.when(self.inner)(f)

        def on_outer(f):
            pl.when(self.outer)(f)

        if s == 0:
            self.ready(k)
            self.go(self.c_core, k)
        elif s == 1:
            for c in self.c_core(k):
                c.wait()
            self.release(0, self.core_peer)
            self.add(k, self.own, r0, 0, self.half)
            self.go(self.c_side, k)
        elif s == 2:
            for c in self.c_side(k):
                c.wait()
            self.add(k, self.a, r1, 0, self.q)
            self.add(k, self.b, r1, self.q, self.q)

            @on_outer
            def _():
                self.go(self.c_in, k)
        elif s == 3:
            @on_inner
            def _():
                self.got(self.c_in, k)
                self.add_both(k, self.to_in, r2, 3 * self.n)
                self.go(self.c_pair, k)

            @on_outer
            def _():
                self.sent(self.c_in, k)
                self.release(1, self.z_inner)
        elif s == 4:
            @on_inner
            def _():
                for c in self.c_pair(k):
                    c.wait()
                self.release(2, self.z_peer)
                self.add_both(k, self.from_pair, r3, 2 * self.n)
                self.go(self.c_end, k)
                self.go(self.c_turn, k)
        elif s == 5:
            @on_inner
            def _():
                self.sent(self.c_end, k)
                self.release(3, self.z_outer)
                self.turn_done(k, r4)
                pl.semaphore_wait(self.free.at[1], 1)
                pl.semaphore_wait(self.free.at[2], 1)
                self.go_lazy(self.c_mine_pair, k)
                self.go_lazy(self.c_mine_out, k)

            @on_outer
            def _():
                self.got(self.c_end, k)
                self.add_both(k, self.mine, r2, self.n)
                self.go(self.c_turn, k)
        elif s == 6:
            @on_inner
            def _():
                self.got(self.c_mine_pair, k)
                self.go_lazy(self.c_twin_out, k)

            @on_outer
            def _():
                self.turn_done(k, r4)
                pl.semaphore_wait(self.free.at[3], 1)
                self.go_lazy(self.c_mine_in, k)
        elif s == 7:
            @on_inner
            def _():
                self.got(self.c_mine_in, k)
                self.go_lazy(self.c_end_pair, k)
        elif s == 8:
            @on_inner
            def _():
                self.got(self.c_end_pair, k)
                self.go_lazy(self.c_far_out, k)
                self.go_lazy(self.c_wide, k)
        elif s == 9:
            @on_outer
            def _():
                self.got(self.c_mine_out, k)
                self.got(self.c_twin_out, k)
                self.got(self.c_far_out, k)
                self.go_lazy(self.c_wide, k)
        elif s == 10:
            self.got(self.c_wide, k)
            pl.semaphore_wait(self.free.at[0], 1)
            self.go_lazy(self.c_full, k)
        elif s == 11:
            self.got(self.c_full, k)
            self.emit(k)

    def tick(self, t):
        for s in reversed(range(len(LAG))):
            k = t - LAG[s]

            @pl.when((k >= 0) & (k < self.total))
            def _():
                self.stage(s, k)

    def drain(self):
        def body(k, _):
            self.sent(self.c_wide, k)
            self.sent(self.c_full, k)

            @pl.when(self.inner)
            def _():
                for make in (self.c_mine_pair, self.c_mine_out, self.c_twin_out, self.c_end_pair, self.c_far_out):
                    self.sent(make, k)

            @pl.when(self.outer)
            def _():
                self.sent(self.c_mine_in, k)
            return 0

        lax.fori_loop(self.total - TURNS, self.total, body, 0)


def backward_kernel(groups, scale, *refs):
    (dw4, g_in, a3, h2, a1, h1, m_in, x0, w4, w3, w2, w1), refs = refs[:12], refs[12:]
    reduced, dm_out, refs = refs[0], refs[1], refs[2:]
    part, r0, r1, r2, r3, r4, d_act, w_down, w_up, g_buf, lhs, dh2, col = refs[:13]
    send, recv, free, load_sem, store_sem, side_sem, col_sem = refs[13:]
    total = 2 * sum(len(blocks_of(g)) for g in groups)

    def load(n, src, dst):
        return pltpu.make_async_copy(src, dst, side_sem.at[n])

    streams = ((a3, 0, 4), (h1, 4, 4), (a1, 8, 4), (x0, 12, 8))

    def fetch(n):
        for ref, first, count in streams:
            @pl.when((n >= first) & (n < first + count))
            def _():
                at = pl.ds(pl.multiple_of((n - first) * SIDE, SIDE), SIDE)
                slot = lax.rem(n, 2)
                pltpu.make_async_copy(ref.at[:, at], col.at[slot], col_sem.at[slot]).start()

    def fetched(n):
        slot = lax.rem(n, 2)
        pltpu.make_async_copy(a3.at[:, pl.ds(0, SIDE)], col.at[slot], col_sem.at[slot]).wait()
        return col.at[slot]

    load(0, g_in, g_buf).start()
    load(1, w4, w_down).start()
    fetch(0)
    load(2, h2, lhs).start()
    fetch(1)
    load(3, w3, w_up).start()
    for k in range(4):
        pltpu.make_async_copy(dw4.at[pl.ds(k * SIDE, SIDE), :], part.at[k], load_sem.at[k]).start()

    def ready(k):
        @pl.when((k < 8) & (lax.rem(k, 2) == 0))
        def _():
            pltpu.make_async_copy(dw4.at[pl.ds(0, SIDE), :], part.at[k // 2], load_sem.at[k // 2]).wait()

    def emit(k):
        rows = pl.ds(pl.multiple_of(lax.rem(k, 2) * UNIT, UNIT), UNIT)
        pltpu.make_async_copy(part.at[k // 2, rows, :], reduced.at[k // 2, rows, :], store_sem.at[k // 2, lax.rem(k, 2)]).start()

    def grad_block(k, left, right, right_cols):
        for piece in range(2):
            rows = pl.ds(piece * 1024, 1024)
            value = rows_contract(left[rows, :], right[rows, right_cols])
            if piece == 0:
                part[k] = value
            else:
                part[k] += value

    def slope_half(at, e, grad, act):
        def body(t, _):
            rows = pl.ds(pl.multiple_of(e * 1024 + t * 256, 256), 256)
            d_out = times_transposed(grad[rows, :], w_down[at, :]).astype(BF16)
            d_act[rows, at] = (d_out.astype(F32) * gelu_slope(act[rows, :])).astype(BF16)
            return 0

        lax.fori_loop(0, 4, body, 0)

    def back_half(e, add, dst):
        def body(t, _):
            rows = pl.ds(pl.multiple_of(e * 1024 + t * 512, 512), 512)
            dst[rows, :] = (times_transposed(d_act[rows, :], w_up[...]) + add[rows, :].astype(F32)).astype(BF16)
            return 0

        lax.fori_loop(0, 2, body, 0)

    def compute(t):
        @pl.when(t == 1)
        def _():
            load(0, g_in, g_buf).wait()
            load(1, w4, w_down).wait()
            load(2, h2, lhs).wait()

        @pl.when(t == 19)
        def _():
            load(4, w2, w_down).wait()
            load(5, m_in, lhs).wait()

        for first, n0, grad, k0 in ((1, 0, g_buf, 4), (19, 8, dh2, 12)):
            @pl.when((t >= first) & (t < first + 12))
            def _():
                j, r = (t - first) // 3, lax.rem(t - first, 3)
                at = pl.ds(pl.multiple_of(j * SIDE, SIDE), SIDE)

                @pl.when(r == 0)
                def _():
                    fetched(n0 + j)

                @pl.when(r < 2)
                def _():
                    slope_half(at, r, grad, col.at[lax.rem(n0 + j, 2)])

                @pl.when(r == 1)
                def _():
                    fetch(n0 + j + 2)

                @pl.when(r == 2)
                def _():
                    grad_block(k0 + j, lhs, d_act, at)

        @pl.when(t == 12)
        def _():
            load(4, w2, w_down).start()
            load(5, m_in, lhs).start()
            load(3, w3, w_up).wait()

        for first, add, dst in ((13, g_buf, dh2), (31, dh2, g_buf)):
            @pl.when((t >= first) & (t < first + 2))
            def _():
                back_half(t - first, add, dst)

        @pl.when(t == 14)
        def _():
            load(6, w1, w_up).start()

        @pl.when(t == 30)
        def _():
            load(6, w1, w_up).wait()

        @pl.when(t == 32)
        def _():
            load(7, g_buf, dm_out).start()

        @pl.when((t >= 15) & (t < 19))
        def _():
            left = fetched(t - 11)
            grad_block(t - 7, left, dh2, slice(None))
            fetch(t - 9)

        @pl.when((t >= 32) & (t < 48) & (lax.rem(t, 2) == 0))
        def _():
            j = (t - 32) // 2
            left = fetched(12 + j)
            grad_block(16 + j, left, g_buf, slice(None))
            fetch(14 + j)

    ex = Exchange(total, scale, part, r0, r1, r2, r3, r4, send, recv, free, ready, emit)
    ex.barrier()

    def step(i, _):
        compute(i)
        ex.tick(i)
        return 0

    lax.fori_loop(0, total + LAG[-1], step, 0)
    ex.drain()
    load(7, g_buf, dm_out).wait()

    def stored(k, _):
        rows = pl.ds(0, UNIT)
        pltpu.make_async_copy(part.at[0, rows, :], reduced.at[0, rows, :], store_sem.at[k // 2, lax.rem(k, 2)]).wait()
        return 0

    lax.fori_loop(0, total, stored, 0)


def backward(dw4, g, a3, h2, a1, h1, m, x0, w4, w3, w2, w1, groups, scale):
    total = sum(len(blocks_of(g)) for g in groups)
    any_spec = pl.BlockSpec(memory_space=pl.ANY)
    rows, wide = a3.shape
    return pl.pallas_call(
        functools.partial(backward_kernel, groups, scale),
        out_shape=[jax.ShapeDtypeStruct((total, SIDE, SIDE), F32), jax.ShapeDtypeStruct((rows, SIDE), BF16)],
        in_specs=[any_spec] * 12,
        out_specs=[any_spec] * 2,
        scratch_shapes=[
            pltpu.VMEM((total, SIDE, SIDE), F32),
            pltpu.VMEM((SLOTS, UNIT // 2, SIDE), F32),
            pltpu.VMEM((SLOTS, UNIT // 4, SIDE), F32),
            pltpu.VMEM((SLOTS, UNIT // 4, SIDE), F32),
            pltpu.VMEM((SLOTS, UNIT // 4, SIDE), F32),
            pltpu.VMEM((SLOTS, UNIT // 16, SIDE), F32),
            pltpu.VMEM((rows, wide), BF16),
            pltpu.VMEM((wide, SIDE), BF16),
            pltpu.VMEM((SIDE, wide), BF16),
            pltpu.VMEM((rows, SIDE), BF16),
            pltpu.VMEM((rows, SIDE), BF16),
            pltpu.VMEM((rows, SIDE), BF16),
            pltpu.VMEM((2, rows, SIDE), BF16),
            pltpu.SemaphoreType.DMA((26, TURNS)),
            pltpu.SemaphoreType.DMA((26, TURNS)),
            pltpu.SemaphoreType.REGULAR((4,)),
            pltpu.SemaphoreType.DMA((4,)),
            pltpu.SemaphoreType.DMA((total, 2)),
            pltpu.SemaphoreType.DMA((8,)),
            pltpu.SemaphoreType.DMA((2,)),
        ],
        compiler_params=pltpu.CompilerParams(
            collective_id=0, has_side_effects=True, vmem_limit_bytes=67 * 1000 * 1000),
        name="backward_and_mean",
    )(dw4, g, a3, h2, a1, h1, m, x0, w4, w3, w2, w1)


def finish_kernel(groups, reduced, dm_in, w0_in, dx, *refs):
    outs, (part, dm, w0, rows_out, load_sem, part_sem, in_sem, dx_sem) = refs[:5], refs[5:]
    loads = (pltpu.make_async_copy(dm_in, dm, in_sem.at[0]), pltpu.make_async_copy(w0_in, w0, in_sem.at[1]))
    for c in loads:
        c.start()
    stores = []
    fetches = [pltpu.make_async_copy(reduced.at[k], part.at[k], load_sem.at[k]) for k in range(part.shape[0])]
    for c in fetches:
        c.start()
    for ref, shape in zip(outs, groups):
        for r, c in blocks_of(shape):
            k = len(stores)
            stores.append(pltpu.make_async_copy(part.at[k], ref.at[pl.ds(r, SIDE), pl.ds(c, SIDE)], part_sem.at[k]))
    steps = w0.shape[0] // SIDE
    each = len(stores) // steps
    for c in loads:
        c.wait()

    def dx_copy(j):
        at = pl.ds(pl.multiple_of(j * SIDE, SIDE), SIDE)
        return pltpu.make_async_copy(rows_out.at[lax.rem(j, 2)], dx.at[:, at], dx_sem.at[lax.rem(j, 2)])

    for j in range(steps):
        for k in range(j * each, (j + 1) * each):
            fetches[k].wait()
            stores[k].start()
        if j >= 2:
            dx_copy(j - 2).wait()

        def piece(i, _):
            at = pl.ds(pl.multiple_of(i * 1024, 1024), 1024)
            rows_out[j % 2, at, :] = times_transposed(dm[at, :], w0[pl.ds(j * SIDE, SIDE), :]).astype(BF16)
            return 0

        lax.fori_loop(0, dm.shape[0] // 1024, piece, 0)
        dx_copy(j).start()
    for j in (steps - 2, steps - 1):
        dx_copy(j).wait()
    for c in stores:
        c.wait()


def finish(reduced, dm, w0, groups):
    any_spec = pl.BlockSpec(memory_space=pl.ANY)
    rows, wide = dm.shape[0], w0.shape[0]
    return pl.pallas_call(
        functools.partial(finish_kernel, groups),
        out_shape=[jax.ShapeDtypeStruct((rows, wide), BF16)] + [jax.ShapeDtypeStruct(g, F32) for g in groups],
        in_specs=[any_spec] * 3,
        out_specs=[any_spec] * 6,
        scratch_shapes=[
            pltpu.VMEM(reduced.shape, F32),
            pltpu.VMEM(dm.shape, BF16),
            pltpu.VMEM(w0.shape, BF16),
            pltpu.VMEM((2, rows, SIDE), BF16),
            pltpu.SemaphoreType.DMA((reduced.shape[0],)),
            pltpu.SemaphoreType.DMA((reduced.shape[0],)),
            pltpu.SemaphoreType.DMA((2,)),
            pltpu.SemaphoreType.DMA((2,)),
        ],
        compiler_params=pltpu.CompilerParams(vmem_limit_bytes=60 * 1000 * 1000),
        name="finish",
    )(reduced, dm, w0)


def solution(mesh):
    batch_axes = ("z", "y", "x")
    scale = 1.0 / mesh.size
    row_spec = P(batch_axes, None)
    full_spec = P(None, None)

    def device_step(x_in, g_out, w_in, w_up1, w_down1, w_up2, w_down2):
        x_mid = plain_product(x_in, w_in).astype(jnp.bfloat16)
        pre_one = plain_product(x_mid, w_up1).astype(jnp.bfloat16)
        act_one = gelu_value(pre_one).astype(jnp.bfloat16)
        hid_two = (plain_product(act_one, w_down1) + x_mid.astype(jnp.float32)).astype(jnp.bfloat16)
        pre_three = plain_product(hid_two, w_up2).astype(jnp.bfloat16)
        act_three = gelu_value(pre_three).astype(jnp.bfloat16)
        dw_down2 = rows_contract(act_three, g_out)
        groups = (dw_down2.shape, w_up2.shape, w_down1.shape, w_up1.shape, w_in.shape)
        reduced, d_mid = backward(
            dw_down2, g_out, pre_three, hid_two, pre_one, act_one, x_mid, x_in, w_down2, w_up2, w_down1, w_up1, groups, scale)
        dx_rows, dw_down2, dw_up2, dw_down1, dw_up1, dw_in = finish(reduced, d_mid, w_in, groups)
        return dx_rows, dw_in, dw_up1, dw_down1, dw_up2, dw_down2

    return jax.shard_map(
        device_step,
        mesh=mesh,
        in_specs=(row_spec, row_spec, full_spec, full_spec, full_spec, full_spec, full_spec),
        out_specs=(row_spec, full_spec, full_spec, full_spec, full_spec, full_spec),
        check_vma=False,
    )
```

```python
import functools
import jax
import jax.numpy as jnp
from jax import lax
from jax.experimental import pallas as pl
from jax.experimental.pallas import tpu as pltpu
from jax.sharding import PartitionSpec as P

SQRT_HALF = 0.7071067811865476
INV_SQRT_TAU = 0.3989422804014327
MESH = pl.DeviceIdType.MESH
F32 = jnp.float32
BF16 = jnp.bfloat16

SIDE = 512
UNIT = SIDE // 2
SLOTS = 8
TURNS = 16
LAG = (0, 1, 4, 6, 8, 11, 13, 14, 16, 19, 23, 25)
TALL = 256


def gelu_value(pre_act):
    pre_wide = pre_act.astype(jnp.float32)
    return 0.5 * pre_wide * (1.0 + lax.erf(pre_wide * SQRT_HALF))


def gelu_slope(pre_act):
    pre_wide = pre_act.astype(jnp.float32)
    return 0.5 * (1.0 + lax.erf(pre_wide * SQRT_HALF)) + pre_wide * jnp.exp(-0.5 * pre_wide * pre_wide) * INV_SQRT_TAU


def plain_product(first_op, second_op):
    return lax.dot_general(first_op, second_op, (((1,), (0,)), ((), ())), preferred_element_type=jnp.float32)


def rows_contract(first_op, second_op):
    return lax.dot_general(first_op, second_op, (((0,), (0,)), ((), ())), preferred_element_type=jnp.float32)


def times_transposed(first_op, second_op):
    return lax.dot_general(first_op, second_op, (((1,), (1,)), ((), ())), preferred_element_type=jnp.float32)


def blocks_of(shape):
    rows, cols = shape
    return [(r, c) for r in range(0, rows, SIDE) for c in range(0, cols, SIDE)]


class Exchange:
    def __init__(self, total, scale, part, r0, r1, r2, r3, r4, send, recv, free, emit):
        self.total, self.scale, self.part = total, scale, part
        self.r0, self.r1, self.r2, self.r3, self.r4 = r0, r1, r2, r3, r4
        self.send, self.recv, self.free, self.emit = send, recv, free, emit
        z, y, x = lax.axis_index("z"), lax.axis_index("y"), lax.axis_index("x")
        core, chip = lax.rem(x, 2), x // 2
        self.core_peer = (z, y, chip * 2 + 1 - core)
        self.x_peer = (z, y, (1 - chip) * 2 + core)
        self.y_peer = (z, 1 - y, x)
        self.inner = (z >= 1) & (z <= 2)
        self.outer = (z == 0) | (z == 3)
        self.z_inner = (jnp.where(z == 0, 1, 2), y, x)
        self.z_peer = (jnp.where(z == 1, 2, 1), y, x)
        self.z_outer = (jnp.where(z == 1, 0, 3), y, x)
        half, self.q = UNIT // 2, UNIT // 8
        n = self.n = self.q // 4
        self.half = half
        self.own = core * half
        self.other = (1 - core) * half
        self.a = self.own + chip * self.q
        self.a_far = self.own + (1 - chip) * self.q
        self.b = self.own + half // 2 + y * self.q
        self.b_far = self.own + half // 2 + (1 - y) * self.q
        high = jnp.where(z >= 2, 1, 0)
        self.to_in = n * (1 - high)
        self.to_pair = 2 * n * (1 - high)
        self.from_pair = 2 * n * high
        self.to_out = 3 * n * high
        self.mine = n * z
        self.twin = n * (3 - z)
        self.far = 3 * n * (1 - high)

    def barrier(self):
        sem = pltpu.get_barrier_semaphore()
        for peer in (self.core_peer, self.x_peer, self.y_peer):
            pl.semaphore_signal(sem, inc=1, device_id=peer, device_id_type=MESH)

        @pl.when(self.inner)
        def _():
            pl.semaphore_signal(sem, inc=1, device_id=self.z_peer, device_id_type=MESH)
            pl.semaphore_signal(sem, inc=1, device_id=self.z_outer, device_id_type=MESH)
            pl.semaphore_wait(sem, 5)

        @pl.when(self.outer)
        def _():
            pl.semaphore_signal(sem, inc=1, device_id=self.z_inner, device_id_type=MESH)
            pl.semaphore_wait(sem, 4)

    def copy(self, kind, k, src, dst, peer):
        turn = lax.rem(k, TURNS)
        return pltpu.make_async_remote_copy(
            src_ref=src, dst_ref=dst, send_sem=self.send.at[kind, turn], recv_sem=self.recv.at[kind, turn],
            device_id=peer, device_id_type=MESH)

    def rows(self, k, start, count):
        at = pl.multiple_of(lax.rem(k, 2) * UNIT + start, 8)
        return self.part.at[k // 2, pl.ds(at, count), :]

    def both(self, kind, k, at, count, peer, into=None):
        slot, out = lax.rem(k, SLOTS), []
        for e, base in enumerate((self.a, self.b)):
            src = self.rows(k, base + at, count)
            dst = src if into is None else into.at[slot, pl.ds(pl.multiple_of(e * self.q + at, 8), count), :]
            out.append(self.copy(kind + e, k, src, dst, peer))
        return out

    def c_core(self, k):
        return [self.copy(0, k, self.rows(k, self.other, self.half), self.r0.at[lax.rem(k, SLOTS)], self.core_peer)]

    def c_side(self, k):
        slot = lax.rem(k, SLOTS)
        return [self.copy(1, k, self.rows(k, self.a_far, self.q), self.r1.at[slot, pl.ds(0, self.q), :], self.x_peer),
                self.copy(2, k, self.rows(k, self.b_far, self.q), self.r1.at[slot, pl.ds(self.q, self.q), :], self.y_peer)]

    def c_in(self, k):
        return self.both(3, k, self.to_in, 3 * self.n, self.z_inner, self.r2)

    def c_pair(self, k):
        return self.both(5, k, self.to_pair, 2 * self.n, self.z_peer, self.r3)

    def c_end(self, k):
        return self.both(7, k, self.to_out, self.n, self.z_outer, self.r2)

    def c_turn(self, k):
        slot, n = lax.rem(k, SLOTS), self.n
        return [self.copy(9, k, self.rows(k, self.a + self.mine, n), self.r4.at[slot, pl.ds(0, n), :], self.y_peer),
                self.copy(10, k, self.rows(k, self.b + self.mine, n), self.r4.at[slot, pl.ds(n, n), :], self.x_peer)]

    def c_mine_pair(self, k):
        return self.both(13, k, self.mine, self.n, self.z_peer)

    def c_mine_out(self, k):
        return self.both(15, k, self.mine, self.n, self.z_outer)

    def c_twin_out(self, k):
        return self.both(17, k, self.twin, self.n, self.z_outer)

    def c_mine_in(self, k):
        return self.both(11, k, self.mine, self.n, self.z_inner)

    def c_end_pair(self, k):
        return self.both(19, k, self.to_out, self.n, self.z_peer)

    def c_far_out(self, k):
        return self.both(21, k, self.far, self.n, self.z_outer)

    def c_wide(self, k):
        a, b = self.rows(k, self.a, self.q), self.rows(k, self.b, self.q)
        return [self.copy(23, k, a, a, self.x_peer), self.copy(24, k, b, b, self.y_peer)]

    def c_full(self, k):
        half = self.rows(k, self.own, self.half)
        return [self.copy(25, k, half, half, self.core_peer)]

    def go(self, make, k):
        for c in make(k):
            c.start()

    def go_lazy(self, make, k):
        @pl.when(k >= TURNS)
        def _():
            for c in make(k - TURNS):
                c.wait_send()

        self.go(make, k)

    def got(self, make, k):
        for c in make(k):
            c.wait_recv()

    def sent(self, make, k):
        for c in make(k):
            c.wait_send()

    def release(self, kind, peer):
        pl.semaphore_signal(self.free.at[kind], inc=1, device_id=peer, device_id_type=MESH)

    def add(self, k, at, src, src_row, count, scale=None):
        base = lax.rem(k, 2) * UNIT + at
        block = k // 2
        step = 16 if count % 16 == 0 else 8
        for i in range(0, count, step):
            rows = pl.ds(pl.multiple_of(base + i, 8), step)
            value = self.part[block, rows, :] + src[pl.ds(pl.multiple_of(src_row + i, 8), step), :]
            self.part[block, rows, :] = value if scale is None else value * scale

    def add_both(self, k, at, src, count):
        for e, base in enumerate((self.a, self.b)):
            self.add(k, base + at, src, e * self.q + at, count)

    def turn_done(self, k, r4):
        for c in self.c_turn(k):
            c.wait()
        self.add(k, self.a + self.mine, r4, 0, self.n, self.scale)
        self.add(k, self.b + self.mine, r4, self.n, self.n, self.scale)

    def stage(self, s, k):
        slot = lax.rem(k, SLOTS)
        r0, r1, r2, r3, r4 = (r.at[slot] for r in (self.r0, self.r1, self.r2, self.r3, self.r4))

        def on_inner(f):
            pl.when(self.inner)(f)

        def on_outer(f):
            pl.when(self.outer)(f)

        if s == 0:
            self.go(self.c_core, k)
        elif s == 1:
            for c in self.c_core(k):
                c.wait()
            self.release(0, self.core_peer)
            self.add(k, self.own, r0, 0, self.half)
            self.go(self.c_side, k)
        elif s == 2:
            for c in self.c_side(k):
                c.wait()
            self.add(k, self.a, r1, 0, self.q)
            self.add(k, self.b, r1, self.q, self.q)

            @on_outer
            def _():
                self.go(self.c_in, k)
        elif s == 3:
            @on_inner
            def _():
                self.got(self.c_in, k)
                self.add_both(k, self.to_in, r2, 3 * self.n)
                self.go(self.c_pair, k)

            @on_outer
            def _():
                self.sent(self.c_in, k)
                self.release(1, self.z_inner)
        elif s == 4:
            @on_inner
            def _():
                for c in self.c_pair(k):
                    c.wait()
                self.release(2, self.z_peer)
                self.add_both(k, self.from_pair, r3, 2 * self.n)
                self.go(self.c_end, k)
                self.go(self.c_turn, k)
        elif s == 5:
            @on_inner
            def _():
                self.sent(self.c_end, k)
                self.release(3, self.z_outer)
                self.turn_done(k, r4)
                pl.semaphore_wait(self.free.at[1], 1)
                pl.semaphore_wait(self.free.at[2], 1)
                self.go_lazy(self.c_mine_pair, k)
                self.go_lazy(self.c_mine_out, k)

            @on_outer
            def _():
                self.got(self.c_end, k)
                self.add_both(k, self.mine, r2, self.n)
                self.go(self.c_turn, k)
        elif s == 6:
            @on_inner
            def _():
                self.got(self.c_mine_pair, k)
                self.go_lazy(self.c_twin_out, k)

            @on_outer
            def _():
                self.turn_done(k, r4)
                pl.semaphore_wait(self.free.at[3], 1)
                self.go_lazy(self.c_mine_in, k)
        elif s == 7:
            @on_inner
            def _():
                self.got(self.c_mine_in, k)
                self.go_lazy(self.c_end_pair, k)
        elif s == 8:
            @on_inner
            def _():
                self.got(self.c_end_pair, k)
                self.go_lazy(self.c_far_out, k)
                self.go_lazy(self.c_wide, k)
        elif s == 9:
            @on_outer
            def _():
                self.got(self.c_mine_out, k)
                self.got(self.c_twin_out, k)
                self.got(self.c_far_out, k)
                self.go_lazy(self.c_wide, k)
        elif s == 10:
            self.got(self.c_wide, k)
            pl.semaphore_wait(self.free.at[0], 1)
            self.go_lazy(self.c_full, k)
        elif s == 11:
            self.got(self.c_full, k)
            self.emit(k)

    def tick(self, t):
        for s in reversed(range(len(LAG))):
            k = t - LAG[s]

            @pl.when((k >= 0) & (k < self.total))
            def _():
                self.stage(s, k)

    def drain(self):
        def body(k, _):
            self.sent(self.c_wide, k)
            self.sent(self.c_full, k)

            @pl.when(self.inner)
            def _():
                for make in (self.c_mine_pair, self.c_mine_out, self.c_twin_out, self.c_end_pair, self.c_far_out):
                    self.sent(make, k)

            @pl.when(self.outer)
            def _():
                self.sent(self.c_mine_in, k)
            return 0

        lax.fori_loop(self.total - TURNS, self.total, body, 0)


def forward_kernel(x, w0, w1, w2, w3, m, a1, h1, h2, a3, h3):
    mid = plain_product(x[...], w0[...]).astype(BF16)
    m[...] = mid
    for c in range(0, w1.shape[1], SIDE):
        at = pl.ds(c, SIDE)
        pre = plain_product(mid, w1[:, at]).astype(BF16)
        a1[:, at] = pre
        h1[:, at] = gelu_value(pre).astype(BF16)
    hid = (plain_product(h1[...], w2[...]) + mid.astype(F32)).astype(BF16)
    h2[...] = hid
    for c in range(0, w3.shape[1], SIDE):
        at = pl.ds(c, SIDE)
        pre = plain_product(hid, w3[:, at]).astype(BF16)
        a3[:, at] = pre
        h3[:, at] = gelu_value(pre).astype(BF16)


def forward(x, w0, w1, w2, w3):
    rows, deep = x.shape
    side, wide = w1.shape
    whole = lambda w: pl.BlockSpec(w.shape, lambda i: (0, 0), pipeline_mode=pl.Buffered(1))
    tile = lambda width: pl.BlockSpec((TALL, width), lambda i: (i, 0))
    widths = (side, wide, wide, side, wide, wide)
    return pl.pallas_call(
        forward_kernel,
        grid=(rows // TALL,),
        out_shape=[jax.ShapeDtypeStruct((rows, n), BF16) for n in widths],
        in_specs=[tile(deep)] + [whole(w) for w in (w0, w1, w2, w3)],
        out_specs=[tile(n) for n in widths],
        compiler_params=pltpu.CompilerParams(vmem_limit_bytes=60 * 1000 * 1000),
        name="forward",
    )(x, w0, w1, w2, w3)


def backward_kernel(groups, scale, *refs):
    (h3, g_in, a3, h2, a1, h1, m_in, x0, w4, w3, w2, w1), refs = refs[:12], refs[12:]
    reduced, dm_out, refs = refs[0], refs[1], refs[2:]
    part, r0, r1, r2, r3, r4, d_act, w_down, w_up, g_buf, lhs, dh2, col, col3 = refs[:14]
    send, recv, free, store_sem, side_sem, col_sem, col3_sem = refs[14:]
    total = 2 * sum(len(blocks_of(g)) for g in groups)

    def load(n, src, dst):
        return pltpu.make_async_copy(src, dst, side_sem.at[n])

    streams = ((a3, 0, 4), (h1, 4, 4), (a1, 8, 4), (x0, 12, 8))

    def fetch(n):
        for ref, first, count in streams:
            @pl.when((n >= first) & (n < first + count))
            def _():
                at = pl.ds(pl.multiple_of((n - first) * SIDE, SIDE), SIDE)
                slot = lax.rem(n, 2)
                pltpu.make_async_copy(ref.at[:, at], col.at[slot], col_sem.at[slot]).start()

    def fetched(n):
        slot = lax.rem(n, 2)
        pltpu.make_async_copy(a3.at[:, pl.ds(0, SIDE)], col.at[slot], col_sem.at[slot]).wait()
        return col.at[slot]

    def h3_copy(j):
        at = pl.ds(pl.multiple_of(j * SIDE, SIDE), SIDE)
        return pltpu.make_async_copy(h3.at[:, at], col3.at[lax.rem(j, 2)], col3_sem.at[lax.rem(j, 2)])

    load(0, g_in, g_buf).start()
    h3_copy(0).start()
    load(1, w4, w_down).start()
    fetch(0)
    h3_copy(1).start()
    load(2, h2, lhs).start()
    fetch(1)
    load(3, w3, w_up).start()

    def emit(k):
        rows = pl.ds(pl.multiple_of(lax.rem(k, 2) * UNIT, UNIT), UNIT)
        pltpu.make_async_copy(part.at[k // 2, rows, :], reduced.at[k // 2, rows, :], store_sem.at[k // 2, lax.rem(k, 2)]).start()

    def grad_block(k, left, right, right_cols):
        for piece in range(2):
            rows = pl.ds(piece * 1024, 1024)
            value = rows_contract(left[rows, :], right[rows, right_cols])
            if piece == 0:
                part[k] = value
            else:
                part[k] += value

    def slope_half(at, e, grad, act):
        def body(t, _):
            rows = pl.ds(pl.multiple_of(e * 1024 + t * 256, 256), 256)
            d_out = times_transposed(grad[rows, :], w_down[at, :]).astype(BF16)
            d_act[rows, at] = (d_out.astype(F32) * gelu_slope(act[rows, :])).astype(BF16)
            return 0

        lax.fori_loop(0, 4, body, 0)

    def back_half(e, add, dst):
        def body(t, _):
            rows = pl.ds(pl.multiple_of(e * 1024 + t * 512, 512), 512)
            dst[rows, :] = (times_transposed(d_act[rows, :], w_up[...]) + add[rows, :].astype(F32)).astype(BF16)
            return 0

        lax.fori_loop(0, 2, body, 0)

    def compute(t):
        @pl.when(t == 0)
        def _():
            load(0, g_in, g_buf).wait()

        @pl.when((t < 8) & (lax.rem(t, 2) == 0))
        def _():
            j = t // 2
            h3_copy(j).wait()
            grad_block(j, col3.at[lax.rem(j, 2)], g_buf, slice(None))

            @pl.when(j < 2)
            def _():
                h3_copy(j + 2).start()

        @pl.when(t == 1)
        def _():
            load(1, w4, w_down).wait()
            load(2, h2, lhs).wait()

        @pl.when(t == 19)
        def _():
            load(4, w2, w_down).wait()
            load(5, m_in, lhs).wait()

        for first, n0, grad, k0 in ((1, 0, g_buf, 4), (19, 8, dh2, 12)):
            @pl.when((t >= first) & (t < first + 12))
            def _():
                j, r = (t - first) // 3, lax.rem(t - first, 3)
                at = pl.ds(pl.multiple_of(j * SIDE, SIDE), SIDE)

                @pl.when(r == 0)
                def _():
                    fetched(n0 + j)

                @pl.when(r < 2)
                def _():
                    slope_half(at, r, grad, col.at[lax.rem(n0 + j, 2)])

                @pl.when(r == 1)
                def _():
                    fetch(n0 + j + 2)

                @pl.when(r == 2)
                def _():
                    grad_block(k0 + j, lhs, d_act, at)

        @pl.when(t == 12)
        def _():
            load(4, w2, w_down).start()
            load(5, m_in, lhs).start()
            load(3, w3, w_up).wait()

        for first, add, dst in ((13, g_buf, dh2), (31, dh2, g_buf)):
            @pl.when((t >= first) & (t < first + 2))
            def _():
                back_half(t - first, add, dst)

        @pl.when(t == 14)
        def _():
            load(6, w1, w_up).start()

        @pl.when(t == 30)
        def _():
            load(6, w1, w_up).wait()

        @pl.when(t == 32)
        def _():
            load(7, g_buf, dm_out).start()

        @pl.when((t >= 15) & (t < 19))
        def _():
            left = fetched(t - 11)
            grad_block(t - 7, left, dh2, slice(None))
            fetch(t - 9)

        @pl.when((t >= 32) & (t < 48) & (lax.rem(t, 2) == 0))
        def _():
            j = (t - 32) // 2
            left = fetched(12 + j)
            grad_block(16 + j, left, g_buf, slice(None))
            fetch(14 + j)

    ex = Exchange(total, scale, part, r0, r1, r2, r3, r4, send, recv, free, emit)
    ex.barrier()

    def step(i, _):
        compute(i)
        ex.tick(i)
        return 0

    lax.fori_loop(0, total + LAG[-1], step, 0)
    ex.drain()
    load(7, g_buf, dm_out).wait()

    def stored(k, _):
        rows = pl.ds(0, UNIT)
        pltpu.make_async_copy(part.at[0, rows, :], reduced.at[0, rows, :], store_sem.at[k // 2, lax.rem(k, 2)]).wait()
        return 0

    lax.fori_loop(0, total, stored, 0)


def backward(h3, g, a3, h2, a1, h1, m, x0, w4, w3, w2, w1, groups, scale):
    total = sum(len(blocks_of(g)) for g in groups)
    any_spec = pl.BlockSpec(memory_space=pl.ANY)
    rows, wide = a3.shape
    return pl.pallas_call(
        functools.partial(backward_kernel, groups, scale),
        out_shape=[jax.ShapeDtypeStruct((total, SIDE, SIDE), F32), jax.ShapeDtypeStruct((rows, SIDE), BF16)],
        in_specs=[any_spec] * 12,
        out_specs=[any_spec] * 2,
        scratch_shapes=[
            pltpu.VMEM((total, SIDE, SIDE), F32),
            pltpu.VMEM((SLOTS, UNIT // 2, SIDE), F32),
            pltpu.VMEM((SLOTS, UNIT // 4, SIDE), F32),
            pltpu.VMEM((SLOTS, UNIT // 4, SIDE), F32),
            pltpu.VMEM((SLOTS, UNIT // 4, SIDE), F32),
            pltpu.VMEM((SLOTS, UNIT // 16, SIDE), F32),
            pltpu.VMEM((rows, wide), BF16),
            pltpu.VMEM((wide, SIDE), BF16),
            pltpu.VMEM((SIDE, wide), BF16),
            pltpu.VMEM((rows, SIDE), BF16),
            pltpu.VMEM((rows, SIDE), BF16),
            pltpu.VMEM((rows, SIDE), BF16),
            pltpu.VMEM((2, rows, SIDE), BF16),
            pltpu.VMEM((2, rows, SIDE), BF16),
            pltpu.SemaphoreType.DMA((26, TURNS)),
            pltpu.SemaphoreType.DMA((26, TURNS)),
            pltpu.SemaphoreType.REGULAR((4,)),
            pltpu.SemaphoreType.DMA((total, 2)),
            pltpu.SemaphoreType.DMA((8,)),
            pltpu.SemaphoreType.DMA((2,)),
            pltpu.SemaphoreType.DMA((2,)),
        ],
        compiler_params=pltpu.CompilerParams(
            collective_id=0, has_side_effects=True, vmem_limit_bytes=67 * 1000 * 1000),
        name="backward_and_mean",
    )(h3, g, a3, h2, a1, h1, m, x0, w4, w3, w2, w1)


def finish_kernel(groups, reduced, dm_in, w0_in, dx, *refs):
    outs, (part, dm, w0, rows_out, load_sem, part_sem, in_sem, dx_sem) = refs[:5], refs[5:]
    loads = (pltpu.make_async_copy(dm_in, dm, in_sem.at[0]), pltpu.make_async_copy(w0_in, w0, in_sem.at[1]))
    for c in loads:
        c.start()
    stores = []
    fetches = [pltpu.make_async_copy(reduced.at[k], part.at[k], load_sem.at[k]) for k in range(part.shape[0])]
    for c in fetches:
        c.start()
    for ref, shape in zip(outs, groups):
        for r, c in blocks_of(shape):
            k = len(stores)
            stores.append(pltpu.make_async_copy(part.at[k], ref.at[pl.ds(r, SIDE), pl.ds(c, SIDE)], part_sem.at[k]))
    steps = w0.shape[0] // SIDE
    each = len(stores) // steps
    for c in loads:
        c.wait()

    def dx_copy(j):
        at = pl.ds(pl.multiple_of(j * SIDE, SIDE), SIDE)
        return pltpu.make_async_copy(rows_out.at[lax.rem(j, 2)], dx.at[:, at], dx_sem.at[lax.rem(j, 2)])

    for j in range(steps):
        for k in range(j * each, (j + 1) * each):
            fetches[k].wait()
            stores[k].start()
        if j >= 2:
            dx_copy(j - 2).wait()

        def piece(i, _):
            at = pl.ds(pl.multiple_of(i * 1024, 1024), 1024)
            rows_out[j % 2, at, :] = times_transposed(dm[at, :], w0[pl.ds(j * SIDE, SIDE), :]).astype(BF16)
            return 0

        lax.fori_loop(0, dm.shape[0] // 1024, piece, 0)
        dx_copy(j).start()
    for j in (steps - 2, steps - 1):
        dx_copy(j).wait()
    for c in stores:
        c.wait()


def finish(reduced, dm, w0, groups):
    any_spec = pl.BlockSpec(memory_space=pl.ANY)
    rows, wide = dm.shape[0], w0.shape[0]
    return pl.pallas_call(
        functools.partial(finish_kernel, groups),
        out_shape=[jax.ShapeDtypeStruct((rows, wide), BF16)] + [jax.ShapeDtypeStruct(g, F32) for g in groups],
        in_specs=[any_spec] * 3,
        out_specs=[any_spec] * 6,
        scratch_shapes=[
            pltpu.VMEM(reduced.shape, F32),
            pltpu.VMEM(dm.shape, BF16),
            pltpu.VMEM(w0.shape, BF16),
            pltpu.VMEM((2, rows, SIDE), BF16),
            pltpu.SemaphoreType.DMA((reduced.shape[0],)),
            pltpu.SemaphoreType.DMA((reduced.shape[0],)),
            pltpu.SemaphoreType.DMA((2,)),
            pltpu.SemaphoreType.DMA((2,)),
        ],
        compiler_params=pltpu.CompilerParams(vmem_limit_bytes=60 * 1000 * 1000),
        name="finish",
    )(reduced, dm, w0)


def solution(mesh):
    batch_axes = ("z", "y", "x")
    scale = 1.0 / mesh.size
    row_spec = P(batch_axes, None)
    full_spec = P(None, None)

    def device_step(x_in, g_out, w_in, w_up1, w_down1, w_up2, w_down2):
        x_mid, pre_one, act_one, hid_two, pre_three, act_three = forward(x_in, w_in, w_up1, w_down1, w_up2)
        groups = (w_down2.shape, w_up2.shape, w_down1.shape, w_up1.shape, w_in.shape)
        reduced, d_mid = backward(
            act_three, g_out, pre_three, hid_two, pre_one, act_one, x_mid, x_in, w_down2, w_up2, w_down1, w_up1, groups, scale)
        dx_rows, dw_down2, dw_up2, dw_down1, dw_up1, dw_in = finish(reduced, d_mid, w_in, groups)
        return dx_rows, dw_in, dw_up1, dw_down1, dw_up2, dw_down2

    return jax.shard_map(
        device_step,
        mesh=mesh,
        in_specs=(row_spec, row_spec, full_spec, full_spec, full_spec, full_spec, full_spec),
        out_specs=(row_spec, full_spec, full_spec, full_spec, full_spec, full_spec),
        check_vma=False,
    )
```

```python
import functools
import jax
import jax.numpy as jnp
from jax import lax
from jax.experimental import pallas as pl
from jax.experimental.pallas import tpu as pltpu
from jax.sharding import PartitionSpec as P

SQRT_HALF = 0.7071067811865476
INV_SQRT_TAU = 0.3989422804014327
MESH = pl.DeviceIdType.MESH
F32 = jnp.float32
BF16 = jnp.bfloat16

SIDE = 512
UNIT = SIDE // 2
SLOTS = 8
TURNS = 16
LAG = (0, 1, 4, 6, 8, 11, 13, 14, 16, 19, 23, 25)
TALL = 256


def gelu_value(pre_act):
    pre_wide = pre_act.astype(jnp.float32)
    return 0.5 * pre_wide * (1.0 + lax.erf(pre_wide * SQRT_HALF))


def gelu_slope(pre_act):
    pre_wide = pre_act.astype(jnp.float32)
    return 0.5 * (1.0 + lax.erf(pre_wide * SQRT_HALF)) + pre_wide * jnp.exp(-0.5 * pre_wide * pre_wide) * INV_SQRT_TAU


def plain_product(first_op, second_op):
    return lax.dot_general(first_op, second_op, (((1,), (0,)), ((), ())), preferred_element_type=jnp.float32)


def rows_contract(first_op, second_op):
    return lax.dot_general(first_op, second_op, (((0,), (0,)), ((), ())), preferred_element_type=jnp.float32)


def times_transposed(first_op, second_op):
    return lax.dot_general(first_op, second_op, (((1,), (1,)), ((), ())), preferred_element_type=jnp.float32)


def blocks_of(shape):
    rows, cols = shape
    return [(r, c) for r in range(0, rows, SIDE) for c in range(0, cols, SIDE)]


class Exchange:
    def __init__(self, total, scale, part, r0, r1, r2, r3, r4, send, recv, free, emit):
        self.total, self.scale, self.part = total, scale, part
        self.r0, self.r1, self.r2, self.r3, self.r4 = r0, r1, r2, r3, r4
        self.send, self.recv, self.free, self.emit = send, recv, free, emit
        z, y, x = lax.axis_index("z"), lax.axis_index("y"), lax.axis_index("x")
        core, chip = lax.rem(x, 2), x // 2
        self.core_peer = (z, y, chip * 2 + 1 - core)
        self.x_peer = (z, y, (1 - chip) * 2 + core)
        self.y_peer = (z, 1 - y, x)
        self.inner = (z >= 1) & (z <= 2)
        self.outer = (z == 0) | (z == 3)
        self.z_inner = (jnp.where(z == 0, 1, 2), y, x)
        self.z_peer = (jnp.where(z == 1, 2, 1), y, x)
        self.z_outer = (jnp.where(z == 1, 0, 3), y, x)
        half, self.q = UNIT // 2, UNIT // 8
        n = self.n = self.q // 4
        self.half = half
        self.own = core * half
        self.other = (1 - core) * half
        self.a = self.own + chip * self.q
        self.a_far = self.own + (1 - chip) * self.q
        self.b = self.own + half // 2 + y * self.q
        self.b_far = self.own + half // 2 + (1 - y) * self.q
        high = jnp.where(z >= 2, 1, 0)
        self.to_in = n * (1 - high)
        self.to_pair = 2 * n * (1 - high)
        self.from_pair = 2 * n * high
        self.to_out = 3 * n * high
        self.mine = n * z
        self.twin = n * (3 - z)
        self.far = 3 * n * (1 - high)

    def barrier(self):
        sem = pltpu.get_barrier_semaphore()
        for peer in (self.core_peer, self.x_peer, self.y_peer):
            pl.semaphore_signal(sem, inc=1, device_id=peer, device_id_type=MESH)

        @pl.when(self.inner)
        def _():
            pl.semaphore_signal(sem, inc=1, device_id=self.z_peer, device_id_type=MESH)
            pl.semaphore_signal(sem, inc=1, device_id=self.z_outer, device_id_type=MESH)
            pl.semaphore_wait(sem, 5)

        @pl.when(self.outer)
        def _():
            pl.semaphore_signal(sem, inc=1, device_id=self.z_inner, device_id_type=MESH)
            pl.semaphore_wait(sem, 4)

    def copy(self, kind, k, src, dst, peer):
        turn = lax.rem(k, TURNS)
        return pltpu.make_async_remote_copy(
            src_ref=src, dst_ref=dst, send_sem=self.send.at[kind, turn], recv_sem=self.recv.at[kind, turn],
            device_id=peer, device_id_type=MESH)

    def rows(self, k, start, count):
        at = pl.multiple_of(lax.rem(k, 2) * UNIT + start, 8)
        return self.part.at[k // 2, pl.ds(at, count), :]

    def both(self, kind, k, at, count, peer, into=None):
        slot, out = lax.rem(k, SLOTS), []
        for e, base in enumerate((self.a, self.b)):
            src = self.rows(k, base + at, count)
            dst = src if into is None else into.at[slot, pl.ds(pl.multiple_of(e * self.q + at, 8), count), :]
            out.append(self.copy(kind + e, k, src, dst, peer))
        return out

    def c_core(self, k):
        return [self.copy(0, k, self.rows(k, self.other, self.half), self.r0.at[lax.rem(k, SLOTS)], self.core_peer)]

    def c_side(self, k):
        slot = lax.rem(k, SLOTS)
        return [self.copy(1, k, self.rows(k, self.a_far, self.q), self.r1.at[slot, pl.ds(0, self.q), :], self.x_peer),
                self.copy(2, k, self.rows(k, self.b_far, self.q), self.r1.at[slot, pl.ds(self.q, self.q), :], self.y_peer)]

    def c_in(self, k):
        return self.both(3, k, self.to_in, 3 * self.n, self.z_inner, self.r2)

    def c_pair(self, k):
        return self.both(5, k, self.to_pair, 2 * self.n, self.z_peer, self.r3)

    def c_end(self, k):
        return self.both(7, k, self.to_out, self.n, self.z_outer, self.r2)

    def c_turn(self, k):
        slot, n = lax.rem(k, SLOTS), self.n
        return [self.copy(9, k, self.rows(k, self.a + self.mine, n), self.r4.at[slot, pl.ds(0, n), :], self.y_peer),
                self.copy(10, k, self.rows(k, self.b + self.mine, n), self.r4.at[slot, pl.ds(n, n), :], self.x_peer)]

    def c_mine_pair(self, k):
        return self.both(13, k, self.mine, self.n, self.z_peer)

    def c_mine_out(self, k):
        return self.both(15, k, self.mine, self.n, self.z_outer)

    def c_twin_out(self, k):
        return self.both(17, k, self.twin, self.n, self.z_outer)

    def c_mine_in(self, k):
        return self.both(11, k, self.mine, self.n, self.z_inner)

    def c_end_pair(self, k):
        return self.both(19, k, self.to_out, self.n, self.z_peer)

    def c_far_out(self, k):
        return self.both(21, k, self.far, self.n, self.z_outer)

    def c_wide(self, k):
        a, b = self.rows(k, self.a, self.q), self.rows(k, self.b, self.q)
        return [self.copy(23, k, a, a, self.x_peer), self.copy(24, k, b, b, self.y_peer)]

    def c_full(self, k):
        half = self.rows(k, self.own, self.half)
        return [self.copy(25, k, half, half, self.core_peer)]

    def go(self, make, k):
        for c in make(k):
            c.start()

    def go_lazy(self, make, k):
        @pl.when(k >= TURNS)
        def _():
            for c in make(k - TURNS):
                c.wait_send()

        self.go(make, k)

    def got(self, make, k):
        for c in make(k):
            c.wait_recv()

    def sent(self, make, k):
        for c in make(k):
            c.wait_send()

    def release(self, kind, peer):
        pl.semaphore_signal(self.free.at[kind], inc=1, device_id=peer, device_id_type=MESH)

    def add(self, k, at, src, src_row, count, scale=None):
        base = lax.rem(k, 2) * UNIT + at
        block = k // 2
        step = 16 if count % 16 == 0 else 8
        for i in range(0, count, step):
            rows = pl.ds(pl.multiple_of(base + i, 8), step)
            value = self.part[block, rows, :] + src[pl.ds(pl.multiple_of(src_row + i, 8), step), :]
            self.part[block, rows, :] = value if scale is None else value * scale

    def add_both(self, k, at, src, count):
        for e, base in enumerate((self.a, self.b)):
            self.add(k, base + at, src, e * self.q + at, count)

    def turn_done(self, k, r4):
        for c in self.c_turn(k):
            c.wait()
        self.add(k, self.a + self.mine, r4, 0, self.n, self.scale)
        self.add(k, self.b + self.mine, r4, self.n, self.n, self.scale)

    def stage(self, s, k):
        slot = lax.rem(k, SLOTS)
        r0, r1, r2, r3, r4 = (r.at[slot] for r in (self.r0, self.r1, self.r2, self.r3, self.r4))

        def on_inner(f):
            pl.when(self.inner)(f)

        def on_outer(f):
            pl.when(self.outer)(f)

        if s == 0:
            self.go(self.c_core, k)
        elif s == 1:
            for c in self.c_core(k):
                c.wait()
            self.release(0, self.core_peer)
            self.add(k, self.own, r0, 0, self.half)
            self.go(self.c_side, k)
        elif s == 2:
            for c in self.c_side(k):
                c.wait()
            self.add(k, self.a, r1, 0, self.q)
            self.add(k, self.b, r1, self.q, self.q)

            @on_outer
            def _():
                self.go(self.c_in, k)
        elif s == 3:
            @on_inner
            def _():
                self.got(self.c_in, k)
                self.add_both(k, self.to_in, r2, 3 * self.n)
                self.go(self.c_pair, k)

            @on_outer
            def _():
                self.sent(self.c_in, k)
                self.release(1, self.z_inner)
        elif s == 4:
            @on_inner
            def _():
                for c in self.c_pair(k):
                    c.wait()
                self.release(2, self.z_peer)
                self.add_both(k, self.from_pair, r3, 2 * self.n)
                self.go(self.c_end, k)
                self.go(self.c_turn, k)
        elif s == 5:
            @on_inner
            def _():
                self.sent(self.c_end, k)
                self.release(3, self.z_outer)
                self.turn_done(k, r4)
                pl.semaphore_wait(self.free.at[1], 1)
                pl.semaphore_wait(self.free.at[2], 1)
                self.go_lazy(self.c_mine_pair, k)
                self.go_lazy(self.c_mine_out, k)

            @on_outer
            def _():
                self.got(self.c_end, k)
                self.add_both(k, self.mine, r2, self.n)
                self.go(self.c_turn, k)
        elif s == 6:
            @on_inner
            def _():
                self.got(self.c_mine_pair, k)
                self.go_lazy(self.c_twin_out, k)

            @on_outer
            def _():
                self.turn_done(k, r4)
                pl.semaphore_wait(self.free.at[3], 1)
                self.go_lazy(self.c_mine_in, k)
        elif s == 7:
            @on_inner
            def _():
                self.got(self.c_mine_in, k)
                self.go_lazy(self.c_end_pair, k)
        elif s == 8:
            @on_inner
            def _():
                self.got(self.c_end_pair, k)
                self.go_lazy(self.c_far_out, k)
                self.go_lazy(self.c_wide, k)
        elif s == 9:
            @on_outer
            def _():
                self.got(self.c_mine_out, k)
                self.got(self.c_twin_out, k)
                self.got(self.c_far_out, k)
                self.go_lazy(self.c_wide, k)
        elif s == 10:
            self.got(self.c_wide, k)
            pl.semaphore_wait(self.free.at[0], 1)
            self.go_lazy(self.c_full, k)
        elif s == 11:
            self.got(self.c_full, k)
            self.emit(k)

    def tick(self, t):
        for s in reversed(range(len(LAG))):
            k = t - LAG[s]

            @pl.when((k >= 0) & (k < self.total))
            def _():
                self.stage(s, k)

    def drain(self):
        def body(k, _):
            self.sent(self.c_wide, k)
            self.sent(self.c_full, k)

            @pl.when(self.inner)
            def _():
                for make in (self.c_mine_pair, self.c_mine_out, self.c_twin_out, self.c_end_pair, self.c_far_out):
                    self.sent(make, k)

            @pl.when(self.outer)
            def _():
                self.sent(self.c_mine_in, k)
            return 0

        lax.fori_loop(self.total - TURNS, self.total, body, 0)


def forward_kernel(x, w0, w1, w2, w3, m, a1, h1, h2, a3, h3):
    mid = plain_product(x[...], w0[...]).astype(BF16)
    m[...] = mid
    for c in range(0, w1.shape[1], SIDE):
        at = pl.ds(c, SIDE)
        pre = plain_product(mid, w1[:, at]).astype(BF16)
        a1[:, at] = pre
        h1[:, at] = gelu_value(pre).astype(BF16)
    hid = (plain_product(h1[...], w2[...]) + mid.astype(F32)).astype(BF16)
    h2[...] = hid
    for c in range(0, w3.shape[1], SIDE):
        at = pl.ds(c, SIDE)
        pre = plain_product(hid, w3[:, at]).astype(BF16)
        a3[:, at] = pre
        h3[:, at] = gelu_value(pre).astype(BF16)


def forward(x, w0, w1, w2, w3):
    rows, deep = x.shape
    side, wide = w1.shape
    whole = lambda w: pl.BlockSpec(w.shape, lambda i: (0, 0), pipeline_mode=pl.Buffered(1))
    tile = lambda width: pl.BlockSpec((TALL, width), lambda i: (i, 0))
    widths = (side, wide, wide, side, wide, wide)
    return pl.pallas_call(
        forward_kernel,
        grid=(rows // TALL,),
        out_shape=[jax.ShapeDtypeStruct((rows, n), BF16) for n in widths],
        in_specs=[tile(deep)] + [whole(w) for w in (w0, w1, w2, w3)],
        out_specs=[tile(n) for n in widths],
        compiler_params=pltpu.CompilerParams(vmem_limit_bytes=60 * 1000 * 1000),
        name="forward",
    )(x, w0, w1, w2, w3)


def backward_kernel(groups, scale, *refs):
    (h3, g_in, a3, h2, a1, h1, m_in, x0, w4, w3, w2, w1), refs = refs[:12], refs[12:]
    reduced, dm_out, refs = refs[0], refs[1], refs[2:]
    part, r0, r1, r2, r3, r4, d_act, w_down, w_up, g_buf, lhs, dh2, col, col3 = refs[:14]
    send, recv, free, store_sem, side_sem, col_sem, col3_sem = refs[14:]
    total = 2 * sum(len(blocks_of(g)) for g in groups)

    def load(n, src, dst):
        return pltpu.make_async_copy(src, dst, side_sem.at[n])

    streams = ((a3, 0, 4), (h1, 4, 4), (a1, 8, 4), (x0, 12, 8))

    def fetch(n):
        for ref, first, count in streams:
            @pl.when((n >= first) & (n < first + count))
            def _():
                at = pl.ds(pl.multiple_of((n - first) * SIDE, SIDE), SIDE)
                slot = lax.rem(n, 2)
                pltpu.make_async_copy(ref.at[:, at], col.at[slot], col_sem.at[slot]).start()

    def fetched(n):
        slot = lax.rem(n, 2)
        pltpu.make_async_copy(a3.at[:, pl.ds(0, SIDE)], col.at[slot], col_sem.at[slot]).wait()
        return col.at[slot]

    def h3_copy(j):
        at = pl.ds(pl.multiple_of(j * SIDE, SIDE), SIDE)
        return pltpu.make_async_copy(h3.at[:, at], col3.at[lax.rem(j, 2)], col3_sem.at[lax.rem(j, 2)])

    load(0, g_in, g_buf).start()
    h3_copy(0).start()
    load(1, w4, w_down).start()
    fetch(0)
    h3_copy(1).start()
    load(2, h2, lhs).start()
    fetch(1)
    load(3, w3, w_up).start()

    def emit(k):
        rows = pl.ds(pl.multiple_of(lax.rem(k, 2) * UNIT, UNIT), UNIT)
        pltpu.make_async_copy(part.at[k // 2, rows, :], reduced.at[k // 2, rows, :], store_sem.at[k // 2, lax.rem(k, 2)]).start()

    def grad_block(k, left, right, right_cols):
        for piece in range(2):
            rows = pl.ds(piece * 1024, 1024)
            value = rows_contract(left[rows, :], right[rows, right_cols])
            if piece == 0:
                part[k] = value
            else:
                part[k] += value

    def slope_half(at, e, grad, act):
        def body(t, _):
            rows = pl.ds(pl.multiple_of(e * 1024 + t * 256, 256), 256)
            d_out = times_transposed(grad[rows, :], w_down[at, :]).astype(BF16)
            d_act[rows, at] = (d_out.astype(F32) * gelu_slope(act[rows, :])).astype(BF16)
            return 0

        lax.fori_loop(0, 4, body, 0, unroll=True)

    def back_half(e, add, dst):
        def body(t, _):
            rows = pl.ds(pl.multiple_of(e * 1024 + t * 512, 512), 512)
            dst[rows, :] = (times_transposed(d_act[rows, :], w_up[...]) + add[rows, :].astype(F32)).astype(BF16)
            return 0

        lax.fori_loop(0, 2, body, 0)

    def compute(t):
        @pl.when(t == 0)
        def _():
            load(0, g_in, g_buf).wait()

        @pl.when((t < 8) & (lax.rem(t, 2) == 0))
        def _():
            j = t // 2
            h3_copy(j).wait()
            grad_block(j, col3.at[lax.rem(j, 2)], g_buf, slice(None))

            @pl.when(j < 2)
            def _():
                h3_copy(j + 2).start()

        @pl.when(t == 1)
        def _():
            load(1, w4, w_down).wait()
            load(2, h2, lhs).wait()

        @pl.when(t == 19)
        def _():
            load(4, w2, w_down).wait()
            load(5, m_in, lhs).wait()

        for first, n0, grad, k0 in ((1, 0, g_buf, 4), (19, 8, dh2, 12)):
            @pl.when((t >= first) & (t < first + 12))
            def _():
                j, r = (t - first) // 3, lax.rem(t - first, 3)
                at = pl.ds(pl.multiple_of(j * SIDE, SIDE), SIDE)

                @pl.when(r == 0)
                def _():
                    fetched(n0 + j)

                @pl.when(r < 2)
                def _():
                    slope_half(at, r, grad, col.at[lax.rem(n0 + j, 2)])

                @pl.when(r == 1)
                def _():
                    fetch(n0 + j + 2)

                @pl.when(r == 2)
                def _():
                    grad_block(k0 + j, lhs, d_act, at)

        @pl.when(t == 12)
        def _():
            load(4, w2, w_down).start()
            load(5, m_in, lhs).start()
            load(3, w3, w_up).wait()

        for first, add, dst in ((13, g_buf, dh2), (31, dh2, g_buf)):
            @pl.when((t >= first) & (t < first + 2))
            def _():
                back_half(t - first, add, dst)

        @pl.when(t == 14)
        def _():
            load(6, w1, w_up).start()

        @pl.when(t == 30)
        def _():
            load(6, w1, w_up).wait()

        @pl.when(t == 32)
        def _():
            load(7, g_buf, dm_out).start()

        @pl.when((t >= 15) & (t < 19))
        def _():
            left = fetched(t - 11)
            grad_block(t - 7, left, dh2, slice(None))
            fetch(t - 9)

        @pl.when((t >= 32) & (t < 48) & (lax.rem(t, 2) == 0))
        def _():
            j = (t - 32) // 2
            left = fetched(12 + j)
            grad_block(16 + j, left, g_buf, slice(None))
            fetch(14 + j)

    ex = Exchange(total, scale, part, r0, r1, r2, r3, r4, send, recv, free, emit)
    ex.barrier()

    def step(i, _):
        compute(i)
        ex.tick(i)
        return 0

    lax.fori_loop(0, total + LAG[-1], step, 0)
    ex.drain()
    load(7, g_buf, dm_out).wait()

    def stored(k, _):
        rows = pl.ds(0, UNIT)
        pltpu.make_async_copy(part.at[0, rows, :], reduced.at[0, rows, :], store_sem.at[k // 2, lax.rem(k, 2)]).wait()
        return 0

    lax.fori_loop(0, total, stored, 0)


def backward(h3, g, a3, h2, a1, h1, m, x0, w4, w3, w2, w1, groups, scale):
    total = sum(len(blocks_of(g)) for g in groups)
    any_spec = pl.BlockSpec(memory_space=pl.ANY)
    rows, wide = a3.shape
    return pl.pallas_call(
        functools.partial(backward_kernel, groups, scale),
        out_shape=[jax.ShapeDtypeStruct((total, SIDE, SIDE), F32), jax.ShapeDtypeStruct((rows, SIDE), BF16)],
        in_specs=[any_spec] * 12,
        out_specs=[any_spec] * 2,
        scratch_shapes=[
            pltpu.VMEM((total, SIDE, SIDE), F32),
            pltpu.VMEM((SLOTS, UNIT // 2, SIDE), F32),
            pltpu.VMEM((SLOTS, UNIT // 4, SIDE), F32),
            pltpu.VMEM((SLOTS, UNIT // 4, SIDE), F32),
            pltpu.VMEM((SLOTS, UNIT // 4, SIDE), F32),
            pltpu.VMEM((SLOTS, UNIT // 16, SIDE), F32),
            pltpu.VMEM((rows, wide), BF16),
            pltpu.VMEM((wide, SIDE), BF16),
            pltpu.VMEM((SIDE, wide), BF16),
            pltpu.VMEM((rows, SIDE), BF16),
            pltpu.VMEM((rows, SIDE), BF16),
            pltpu.VMEM((rows, SIDE), BF16),
            pltpu.VMEM((2, rows, SIDE), BF16),
            pltpu.VMEM((2, rows, SIDE), BF16),
            pltpu.SemaphoreType.DMA((26, TURNS)),
            pltpu.SemaphoreType.DMA((26, TURNS)),
            pltpu.SemaphoreType.REGULAR((4,)),
            pltpu.SemaphoreType.DMA((total, 2)),
            pltpu.SemaphoreType.DMA((8,)),
            pltpu.SemaphoreType.DMA((2,)),
            pltpu.SemaphoreType.DMA((2,)),
        ],
        compiler_params=pltpu.CompilerParams(
            collective_id=0, has_side_effects=True, vmem_limit_bytes=67 * 1000 * 1000),
        name="backward_and_mean",
    )(h3, g, a3, h2, a1, h1, m, x0, w4, w3, w2, w1)


def finish_kernel(groups, reduced, dm_in, w0_in, dx, *refs):
    outs, (part, dm, w0, rows_out, load_sem, part_sem, in_sem, dx_sem) = refs[:5], refs[5:]
    loads = (pltpu.make_async_copy(dm_in, dm, in_sem.at[0]), pltpu.make_async_copy(w0_in, w0, in_sem.at[1]))
    for c in loads:
        c.start()
    stores = []
    fetches = [pltpu.make_async_copy(reduced.at[k], part.at[k], load_sem.at[k]) for k in range(part.shape[0])]
    for c in fetches:
        c.start()
    for ref, shape in zip(outs, groups):
        for r, c in blocks_of(shape):
            k = len(stores)
            stores.append(pltpu.make_async_copy(part.at[k], ref.at[pl.ds(r, SIDE), pl.ds(c, SIDE)], part_sem.at[k]))
    steps = w0.shape[0] // SIDE
    each = len(stores) // steps
    for c in loads:
        c.wait()

    def dx_copy(j):
        at = pl.ds(pl.multiple_of(j * SIDE, SIDE), SIDE)
        return pltpu.make_async_copy(rows_out.at[lax.rem(j, 2)], dx.at[:, at], dx_sem.at[lax.rem(j, 2)])

    for j in range(steps):
        for k in range(j * each, (j + 1) * each):
            fetches[k].wait()
            stores[k].start()
        if j >= 2:
            dx_copy(j - 2).wait()

        def piece(i, _):
            at = pl.ds(pl.multiple_of(i * 1024, 1024), 1024)
            rows_out[j % 2, at, :] = times_transposed(dm[at, :], w0[pl.ds(j * SIDE, SIDE), :]).astype(BF16)
            return 0

        lax.fori_loop(0, dm.shape[0] // 1024, piece, 0)
        dx_copy(j).start()
    for j in (steps - 2, steps - 1):
        dx_copy(j).wait()
    for c in stores:
        c.wait()


def finish(reduced, dm, w0, groups):
    any_spec = pl.BlockSpec(memory_space=pl.ANY)
    rows, wide = dm.shape[0], w0.shape[0]
    return pl.pallas_call(
        functools.partial(finish_kernel, groups),
        out_shape=[jax.ShapeDtypeStruct((rows, wide), BF16)] + [jax.ShapeDtypeStruct(g, F32) for g in groups],
        in_specs=[any_spec] * 3,
        out_specs=[any_spec] * 6,
        scratch_shapes=[
            pltpu.VMEM(reduced.shape, F32),
            pltpu.VMEM(dm.shape, BF16),
            pltpu.VMEM(w0.shape, BF16),
            pltpu.VMEM((2, rows, SIDE), BF16),
            pltpu.SemaphoreType.DMA((reduced.shape[0],)),
            pltpu.SemaphoreType.DMA((reduced.shape[0],)),
            pltpu.SemaphoreType.DMA((2,)),
            pltpu.SemaphoreType.DMA((2,)),
        ],
        compiler_params=pltpu.CompilerParams(vmem_limit_bytes=60 * 1000 * 1000),
        name="finish",
    )(reduced, dm, w0)


def solution(mesh):
    batch_axes = ("z", "y", "x")
    scale = 1.0 / mesh.size
    row_spec = P(batch_axes, None)
    full_spec = P(None, None)

    def device_step(x_in, g_out, w_in, w_up1, w_down1, w_up2, w_down2):
        x_mid, pre_one, act_one, hid_two, pre_three, act_three = forward(x_in, w_in, w_up1, w_down1, w_up2)
        groups = (w_down2.shape, w_up2.shape, w_down1.shape, w_up1.shape, w_in.shape)
        reduced, d_mid = backward(
            act_three, g_out, pre_three, hid_two, pre_one, act_one, x_mid, x_in, w_down2, w_up2, w_down1, w_up1, groups, scale)
        dx_rows, dw_down2, dw_up2, dw_down1, dw_up1, dw_in = finish(reduced, d_mid, w_in, groups)
        return dx_rows, dw_in, dw_up1, dw_down1, dw_up2, dw_down2

    return jax.shard_map(
        device_step,
        mesh=mesh,
        in_specs=(row_spec, row_spec, full_spec, full_spec, full_spec, full_spec, full_spec),
        out_specs=(row_spec, full_spec, full_spec, full_spec, full_spec, full_spec),
        check_vma=False,
    )
```
